512 devices in a mesh: members: 2 (over y), patch: 64 (over z, core), feat: 4 (over x).
Axes of the slice: x: 4, y: 2, z: 32, core: 2. Of those that a mesh axis runs over, the one named last changes fastest.
The devices are a block of a 4x8x32 slice.
Arguments:
- latents: bfloat16 [393216, 512], P(('members', 'patch', 'feat')), parts along dimension 0, may hold values from -6 to 6
- neighbours: int32 [196608, 8], P(('patch', 'feat')), may hold values from 0 to 1279
- degree: int32 [196608], P(('patch', 'feat')), may hold values from 4 to 8
- send_rows: int32 [16384, 8], P(('patch', 'feat')), may hold values from 0 to 767
- area: float32 [196608], P(('patch', 'feat')), may hold values from 0.3 to 10
- scenario: int32 [6], P('members'), parts along dimension 0, may hold values from 0 to 15
- totals: float32 [16, 3], replicated, may hold values from 0.3 to 1.5
- w_send: bfloat16 [1, 512, 512], P(None, None, 'feat'), may hold values from -0.25 to 0.25
- w_recv: bfloat16 [1, 512, 512], P(None, None, 'feat'), may hold values from -0.25 to 0.25
- b_edge: float32 [1, 512], replicated, may hold values from -3 to 3
- w_msg: bfloat16 [1, 512, 512], P(None, None, 'feat'), may hold values from -0.25 to 0.25
- w_node: bfloat16 [1, 1024, 512], P(None, None, 'feat'), may hold values from -0.1875 to 0.1875
- w_out: bfloat16 [1, 512, 512], P(None, None, 'feat'), may hold values from -0.25 to 0.25
- gain: float32 [1, 512], replicated, may hold values from 0.5 to 1.5
- w_dec: bfloat16 [3, 512], replicated, may hold values from -0.25 to 0.25
- w_enc: float32 [3, 512], replicated, may hold values from -3 to 3
Outputs:
- final_latents: bfloat16 [393216, 512], P(('members', 'patch', 'feat')), parts along dimension 0
- conserved: float32 [4, 3, 196608], P('members', None, ('patch', 'feat')), parts along dimension 0
The draws below stay inside these ranges and needn't reach their ends.
There are 2 independent parts, one for each index of `members`. The reference program is written for one: setup_inputs(seed, part) draws one part's arguments, and reference() takes and returns one part's arrays. A program takes and returns all parts, laid end to end along the dimension named above; an argument that names none is the same for every part. Nothing has to cross between parts.
Inputs may be any that keep to these rules, and one draw needn't show every extreme that they name: `neighbours`: an entry below 768 is a row of the node's own device; entry 768 + j * 8 + t names the t-th row that the device of patch j with the same feat index sends to the node's patch. A node's live slots are its first degree[n] slots. `send_rows`: row q * 64 + i lists rows of device q, in its own numbering, that patch i receives.
All inputs are finite; a program needn't handle non-finite values.
Results may differ from the reference program's by a relative error of at most 0.012.
Values may be sent and summed in bfloat16 or wider, within the bound.
A program may use at most 64 MiB of HBM per device.

```python
import math
import jax
import jax.numpy as jnp
from jax import lax

D = 512
NODE_DEV = 768
DEG = 8
SLOT = 8
LAYERS = 1
STEPS = 2
FIELDS = 3
SCEN = 16
NODES = 196608
N_PATCH = 64
N_FEAT = 4


def draw_area(key, part):
    position = jnp.arange(NODES, dtype=jnp.float32) / NODES
    baseline = 1.0 + 2.0 * position
    level_key = jax.random.fold_in(key, 7)
    level = jnp.exp(jax.random.uniform(level_key, (), jnp.float32, -0.5, 0.5))
    rough = jnp.exp(jax.random.uniform(key, (NODES,), jnp.float32, -0.69, 0.69))
    return (level * baseline * rough).astype(jnp.float32)


def plant(array, own_key, least, high):
    longest = array.shape.index(max(array.shape))
    spots = []
    for shift in (0, 1):
        where = [jax.random.randint(jax.random.fold_in(own_key, axis), (), 0, length) for axis, length in enumerate(array.shape)]
        where[longest] = (where[longest] + shift) % array.shape[longest]
        spots.append(tuple(where))
    return array.at[spots[0]].set(least).at[spots[1]].set(high)


def block_levels(own_key, shape, shards, least, high):
    loudness, own = 1.0, jax.random.fold_in(own_key, 6)
    for axis_at, shards_of in shards:
        draws = jnp.exp(jax.random.uniform(jax.random.fold_in(own, axis_at), (shards_of,), jnp.float32, least / len(shards), high / len(shards)))
        loudness = loudness * jnp.repeat(draws, shape[axis_at] // shards_of).reshape([-1 if axis == axis_at else 1 for axis in range(len(shape))])
    return loudness


def scatter_about(stream_key, shape, width, reach, cuts=(), held_as=jnp.bfloat16):
    result = jax.random.normal(stream_key, shape, jnp.float32) * width
    if len(cuts) > 0:
        result = block_levels(stream_key, shape, cuts, -0.22, 0.18) * result
    return jnp.clip(result, min=-reach, max=reach).astype(held_as)


def setup_inputs(seed: int = 0, part: int = 0) -> dict:
    keys = jax.random.split(jax.random.key(seed), 17)
    part_splits = jax.random.split(jax.random.fold_in(keys[16], part), 17)
    return {
        "latents": scatter_about(part_splits[0], (NODES, D), 1.0, 6.0, ((0, 256),)),
        "neighbours": plant(jax.random.randint(keys[1], (NODES, DEG), 0, NODE_DEV + N_PATCH * SLOT), jax.random.fold_in(keys[1], 1), 0, (NODE_DEV + N_PATCH * SLOT) - 1).astype(jnp.int32),
        "degree": plant(jax.random.randint(keys[2], (NODES,), 4, DEG + 1), jax.random.fold_in(keys[2], 1), 4, DEG).astype(jnp.int32),
        "send_rows": plant(jax.random.randint(keys[3], (N_PATCH * N_FEAT * N_PATCH, SLOT), 0, NODE_DEV), jax.random.fold_in(keys[3], 1), 0, NODE_DEV - 1).astype(jnp.int32),
        "area": draw_area(jax.random.fold_in(keys[16], 71), part),
        "scenario": jax.random.randint(part_splits[5], (FIELDS,), 0, SCEN).astype(jnp.int32),
        "totals": jnp.clip(jnp.exp(jax.random.uniform(keys[6], (SCEN, FIELDS), jnp.float32, math.log(0.3), math.log(1.5))), 0.3, 1.5),
        "w_send": scatter_about(keys[7], (LAYERS, D, D), D ** -0.5, 0.25, ((2, 4),)),
        "w_recv": scatter_about(keys[8], (LAYERS, D, D), D ** -0.5, 0.25, ((2, 4),)),
        "b_edge": scatter_about(keys[9], (LAYERS, D), 0.5, 3.0, (), jnp.float32),
        "w_msg": scatter_about(keys[10], (LAYERS, D, D), D ** -0.5, 0.25, ((2, 4),)),
        "w_node": scatter_about(keys[11], (LAYERS, 2 * D, D), (2 * D) ** -0.5, 0.1875, ((2, 4),)),
        "w_out": scatter_about(keys[12], (LAYERS, D, D), D ** -0.5, 0.25, ((2, 4),)),
        "gain": jnp.clip(1.0 + 0.1 * jax.random.normal(keys[13], (LAYERS, D), jnp.float32), 0.5, 1.5),
        "w_dec": scatter_about(keys[14], (FIELDS, D), D ** -0.5, 0.25),
        "w_enc": scatter_about(keys[15], (FIELDS, D), 0.5, 3.0, (), jnp.float32),
    }


EPSILON = 1e-05

def sender_ids(neighbours, send_rows):
    device = (jnp.arange(NODES, dtype=jnp.int32) // NODE_DEV)[:, None]
    node_patch = device // N_FEAT
    node_feat = device % N_FEAT
    is_local = neighbours < NODE_DEV
    remote = jnp.maximum(neighbours - NODE_DEV, 0)
    source = (remote // SLOT).astype(jnp.int32)
    within = (remote % SLOT).astype(jnp.int32)
    source_dev = source * N_FEAT + node_feat
    sent_row = send_rows[source_dev * N_PATCH + node_patch, within]
    return jnp.where(is_local, device * NODE_DEV + neighbours, source_dev * NODE_DEV + sent_row).astype(jnp.int32)

def layer_update(latent, senders, live_slots, weight_send, weight_recv, bias_edge, weight_msg, weight_node, weight_out, gain_row):
    sender = jnp.dot(latent, weight_send, preferred_element_type=jnp.float32).astype(jnp.bfloat16)
    receiver = jnp.dot(latent, weight_recv, preferred_element_type=jnp.float32) + bias_edge
    summed = jnp.zeros((NODES, D), jnp.float32)
    for position in range(DEG):
        edge_value = sender[senders[:, position]].astype(jnp.float32) + receiver
        summed = summed + jnp.where(live_slots[:, position:position + 1], jax.nn.silu(edge_value), 0.0)
    summed = summed.astype(jnp.bfloat16)
    message = jnp.dot(summed, weight_msg, preferred_element_type=jnp.float32).astype(jnp.bfloat16)
    hidden = jax.nn.silu(jnp.dot(latent, weight_node[:D], preferred_element_type=jnp.float32) + jnp.dot(message, weight_node[D:], preferred_element_type=jnp.float32)).astype(jnp.bfloat16)
    output = jnp.dot(hidden, weight_out, preferred_element_type=jnp.float32)
    average = lax.optimization_barrier(jnp.mean(output, axis=1, keepdims=True))
    variance = lax.optimization_barrier(jnp.mean(jnp.square(output - average), axis=1, keepdims=True))
    normed = (output - average) * lax.rsqrt(variance + EPSILON) * gain_row
    return (latent.astype(jnp.float32) + normed).astype(jnp.bfloat16)

def reference(latents, neighbours, degree, send_rows, area, scenario, totals, w_send, w_recv, b_edge, w_msg, w_node, w_out, gain, w_dec, w_enc):
    senders = sender_ids(neighbours, send_rows)
    live_slots = jnp.arange(DEG, dtype=jnp.int32)[None, :] < degree[:, None]
    chosen = (jnp.arange(SCEN, dtype=jnp.int32)[:, None] == scenario[None, :]).astype(jnp.float32)
    target = lax.optimization_barrier(jnp.sum(chosen * totals, axis=0))
    latent_state = latents
    history = []
    for step_index in range(STEPS):
        for layer_index in range(LAYERS):
            latent_state = layer_update(latent_state, senders, live_slots, w_send[layer_index], w_recv[layer_index], b_edge[layer_index], w_msg[layer_index], w_node[layer_index], w_out[layer_index], gain[layer_index])
        decoded = lax.dot_general(w_dec, latent_state, (((1,), (1,)), ((), ())), preferred_element_type=jnp.float32)
        fields = jax.nn.softplus(decoded)
        integral = lax.optimization_barrier(jnp.sum(area[None, :] * fields, axis=1))
        scale = target * float(NODES) / integral
        history.append(scale[:, None] * fields)
        change = (scale - 1.0)[:, None] * fields
        update = lax.dot_general(change, w_enc, (((0,), (0,)), ((), ())), precision=lax.Precision.HIGHEST, preferred_element_type=jnp.float32)
        latent_state = (latent_state.astype(jnp.float32) + update).astype(jnp.bfloat16)
    return (latent_state, jnp.stack(history))
```

```python
import functools

import jax
import jax.numpy as jnp
from jax import lax
from jax.experimental import pallas as pl
from jax.experimental.pallas import tpu as pltpu
from jax.sharding import PartitionSpec as P

STEPS = 2
EPSILON = 1e-05
DEAD = -1e30
MESH = pl.DeviceIdType.MESH
F32 = jnp.float32
BF16 = jnp.bfloat16
NT = (((1,), (1,)), ((), ()))


def mm(a, b):
    return jnp.dot(a, b, preferred_element_type=F32)


def half_silu(half):
    return half * jnp.tanh(half) + half


def softplus(x):
    return jnp.maximum(x, 0.0) + jnp.log1p(jnp.exp(-jnp.abs(x)))


def kernel(
    n_patch,
    n_feat,
    h_ref,
    nbr_ref,
    deg_ref,
    rows_ref,
    area_ref,
    scen_ref,
    tot_ref,
    ws_ref,
    wr_ref,
    be_ref,
    wm_ref,
    wn_ref,
    wo_ref,
    gain_ref,
    wd_ref,
    we_ref,
    out_ref,
    cons_ref,
    w,
    ids,
    ohs,
    ohl,
    ohf,
    ohn,
    pre,
    acc,
    table,
    recv_half,
    h_node,
    h_next,
    send,
    recv,
    ar_src,
    ar_all,
    ax_src,
    ax_all,
    wl_sem,
    ws_sem,
    wr_sem,
    fs_sem,
    fr_sem,
    as_sem,
    ar_sem,
    ps_sem,
    pr_sem,
    xs_sem,
    xr_sem,
):
    nodes, width = h_ref.shape
    deg = nbr_ref.shape[0]
    slot = rows_ref.shape[0]
    blocks, block = acc.shape[0], acc.shape[1]
    cols = ws_ref.shape[2]
    half = n_patch // 2
    quarter = n_patch // 4
    fan = half * slot
    pieces = w.shape[0]
    me = lax.axis_index("patch")
    feat = lax.axis_index("feat")
    core = lax.rem(me, 2)
    partner = me + 1 - 2 * core

    def peer(offset):
        return lax.rem(me + offset, n_patch)

    def side(offset):
        return lax.rem(feat + offset, n_feat)

    barrier = pltpu.get_barrier_semaphore()

    def greet(offset, carry):
        pl.semaphore_signal(barrier, inc=1, device_id={"patch": peer(offset)}, device_id_type=MESH)
        return carry

    for offset in range(1, n_feat):
        pl.semaphore_signal(barrier, inc=1, device_id={"feat": side(offset)}, device_id_type=MESH)
    lax.fori_loop(1, n_patch, greet, 0)

    span = width // 2
    mine = pl.ds(pl.multiple_of(core * span, span), span)
    own_cols = pl.ds(pl.multiple_of(feat * cols, cols), cols)
    low = pl.ds(pl.multiple_of(core * span, span), span)
    high = pl.ds(pl.multiple_of(width + core * span, span), span)
    shards = (
        ws_ref.at[0, low],
        wr_ref.at[0, low],
        wn_ref.at[0, low],
        wm_ref.at[0, low],
        wn_ref.at[0, high],
        wo_ref.at[0, low],
    )
    local = [
        pltpu.make_async_copy(shards[i], w.at[i, mine, own_cols], wl_sem.at[i])
        for i in range(pieces)
    ]
    for copy in local:
        copy.start()

    picks = rows_ref[...].T.astype(F32)
    total_rows = n_patch * slot
    spread = jnp.where(
        lax.broadcasted_iota(jnp.int32, (total_rows, n_patch), 0) // slot
        == lax.broadcasted_iota(jnp.int32, (total_rows, n_patch), 1),
        1.0,
        0.0,
    ).astype(BF16)
    coarse = jnp.floor(picks * (1.0 / 16.0))
    fine = picks - 16.0 * coarse
    each = mm(spread, coarse.astype(BF16)) * 16.0 + mm(spread, fine.astype(BF16))
    lane = lax.broadcasted_iota(jnp.int32, (total_rows, slot), 1)
    turn = lax.broadcasted_iota(jnp.int32, (total_rows, slot), 0) % slot
    chosen_row = jnp.sum(jnp.where(lane == turn, each, 0.0), axis=1, keepdims=True)
    node_at = lax.broadcasted_iota(jnp.int32, (total_rows, nodes), 1).astype(F32)
    ohs[...] = jnp.where(chosen_row == node_at, 1.0, 0.0).astype(BF16)

    def fill_send(step, source):
        picked = mm(ohs[...], source).astype(BF16).reshape(n_patch, slot, width)
        send[step] = picked
        recv[step, pl.ds(quarter, 1)] = send[step, pl.ds(me, 1)]

    fill_send(0, h_ref[...])

    pl.semaphore_wait(barrier, n_patch - 1 + n_feat - 1)

    def exchange(step, offset, group):
        target = peer(offset)
        place = lax.rem(n_patch - offset + quarter, n_patch)
        pltpu.make_async_remote_copy(
            src_ref=send.at[step, target],
            dst_ref=recv.at[step, place],
            send_sem=as_sem.at[step],
            recv_sem=ar_sem.at[step, group],
            device_id={"patch": target},
            device_id_type=MESH,
        ).start()

    def start_exchange(step):
        def pair(group):
            def body(j, carry):
                exchange(step, half - j, group)
                exchange(step, half + j, group)
                return carry

            return body

        exchange(step, half, 1)
        lax.fori_loop(1, quarter, pair(1), 0)
        exchange(step, half + quarter, 1)
        exchange(step, quarter, 0)
        lax.fori_loop(quarter + 1, half, pair(0), 0)

    def wait_far(step):
        ref = recv.at[step, pl.ds(half, half)]
        pltpu.make_async_copy(ref, ref, ar_sem.at[step, 1]).wait()

    def wait_near(step):
        ref = recv.at[step, pl.ds(0, half - 1)]
        pltpu.make_async_copy(ref, ref, ar_sem.at[step, 0]).wait()

    start_exchange(0)

    def shard_copy(i, offset):
        return pltpu.make_async_remote_copy(
            src_ref=w.at[i, mine, own_cols],
            dst_ref=w.at[i, mine, own_cols],
            send_sem=ws_sem.at[i, offset - 1],
            recv_sem=wr_sem.at[i, offset - 1],
            device_id={"feat": side(offset)},
            device_id_type=MESH,
        )

    for i in range(pieces):
        local[i].wait()
        for offset in range(1, n_feat):
            shard_copy(i, offset).start()

    def swap_copy(i):
        return pltpu.make_async_remote_copy(
            src_ref=w.at[i, mine],
            dst_ref=w.at[i, mine],
            send_sem=fs_sem.at[i],
            recv_sem=fr_sem.at[i],
            device_id={"patch": partner},
            device_id_type=MESH,
        )

    def pass_on(i):
        for offset in range(1, n_feat):
            shard_copy(i, offset).wait_recv()
        swap_copy(i).start()

    raw = nbr_ref[...]
    far_id = jnp.maximum(raw - nodes, 0)
    place = far_id // slot - me + quarter
    place = jnp.where(place < 0, place + n_patch, place)
    place = jnp.where(place >= n_patch, place - n_patch, place)
    ordered = jnp.where(raw < nodes, raw, nodes + place * slot + far_id % slot)
    live = lax.broadcasted_iota(jnp.int32, raw.shape, 0) < deg_ref[...]
    ids[...] = jnp.where(live, ordered, -1).T

    def select(b, carry):
        rows = pl.ds(b * block, block)
        mine_ids = ids[rows]
        for k in range(deg):
            col = mine_ids[:, k : k + 1]
            at = b * deg + k
            for ref, base in ((ohl, 0), (ohn, nodes), (ohf, nodes + fan)):
                here = lax.broadcasted_iota(jnp.int32, ref.shape[1:], 1) + base
                ref[at] = jnp.where(col == here, 1.0, 0.0).astype(BF16)
        return carry

    lax.fori_loop(0, blocks, select, 0)

    fields = wd_ref.shape[0]
    nodes_all = float(nodes * n_patch * n_feat)
    scenario_at = lax.broadcasted_iota(jnp.int32, tot_ref.shape, 0)
    target = jnp.sum(jnp.where(scenario_at == scen_ref[...], tot_ref[...], 0.0), axis=0, keepdims=True)
    diagonal = lax.broadcasted_iota(jnp.int32, (fields, fields), 0) == lax.broadcasted_iota(
        jnp.int32, (fields, fields), 1
    )
    lanes = ar_src.shape[2]

    def start_sum(step, local_fields):
        part = jnp.sum(local_fields * area_ref[...], axis=1, keepdims=True)
        wide = jnp.broadcast_to(part, (fields, lanes))
        mark = lax.broadcasted_iota(jnp.int32, (fields, lanes), 0) == lax.broadcasted_iota(
            jnp.int32, (fields, lanes), 1
        )
        line = jnp.sum(jnp.where(mark, wide, 0.0), axis=0, keepdims=True)
        ar_src[step] = line
        ar_all[step, pl.ds(me, 1)] = line.reshape(1, 1, lanes)

        def one(offset):
            pltpu.make_async_remote_copy(
                src_ref=ar_src.at[step],
                dst_ref=ar_all.at[step, me],
                send_sem=ps_sem.at[step],
                recv_sem=pr_sem.at[step],
                device_id={"patch": peer(offset)},
                device_id_type=MESH,
            ).start()

        def both(j, carry):
            one(half - j)
            one(half + j)
            return carry

        one(half)
        lax.fori_loop(1, half, both, 0)

    def side_copy(step, offset):
        return pltpu.make_async_remote_copy(
            src_ref=ax_src.at[step],
            dst_ref=ax_all.at[step, feat],
            send_sem=xs_sem.at[step, offset - 1],
            recv_sem=xr_sem.at[step, offset - 1],
            device_id={"feat": side(offset)},
            device_id_type=MESH,
        )

    def finish_sum(step):
        ref = ar_all.at[step, pl.ds(0, n_patch - 1)]
        pltpu.make_async_copy(ref, ref, pr_sem.at[step]).wait()
        line = jnp.sum(ar_all[step], axis=0)
        ax_src[step] = line
        ax_all[step, pl.ds(feat, 1)] = line.reshape(1, 1, lanes)
        for offset in range(1, n_feat):
            side_copy(step, offset).start()
        for offset in range(1, n_feat):
            side_copy(step, offset).wait_recv()
        integral = jnp.sum(ax_all[step], axis=0)[:, :fields]
        scale = target * nodes_all / integral
        wide = jnp.broadcast_to(scale, (fields, fields))
        return jnp.sum(jnp.where(diagonal, wide, 0.0), axis=1, keepdims=True)

    wd = wd_ref[...]

    def rescaled(rows, mix):
        part = softplus(lax.dot_general(rows, wd, NT, preferred_element_type=F32))
        change = jnp.dot(part, mix, precision=lax.Precision.HIGHEST, preferred_element_type=F32)
        return (rows.astype(F32) + change).astype(BF16)

    def project(b, carry):
        rows = pl.ds(b * block, block)
        latent = h_next[rows]
        table[rows] = (0.5 * mm(latent, w[0])).astype(BF16)
        recv_half[b] = 0.5 * (mm(latent, w[1]) + be_ref[...])
        return carry

    def local_edges(b, carry):
        mine_ids = ids[pl.ds(b * block, block)]
        base = recv_half[b]
        for k in range(deg):
            dead = jnp.where(mine_ids[:, k : k + 1] < 0, DEAD, 0.0)
            at = b * deg + k
            pre[at] = mm(ohl[at], table[pl.ds(0, nodes)]) + (base + dead)
        return carry

    def node_part(b, carry):
        h_node[b] = mm(h_next[pl.ds(b * block, block)], w[2])
        return carry

    def far_edges(i, carry):
        pre[i] += mm(ohf[i], table[pl.ds(nodes + fan, fan)])
        return carry

    def finish_block(b, carry):
        total = jnp.zeros((block, width), F32)
        for k in range(deg):
            at = b * deg + k
            total = total + half_silu(pre[at] + mm(ohn[at], table[pl.ds(nodes, fan)]))
        message = mm(total.astype(BF16), w[3]).astype(BF16)
        hidden = half_silu(0.5 * (h_node[b] + mm(message, w[4]))).astype(BF16)
        output = mm(hidden, w[5])
        average = jnp.mean(output, axis=1, keepdims=True)
        centred = output - average
        variance = jnp.mean(jnp.square(centred), axis=1, keepdims=True)
        normed = centred * lax.rsqrt(variance + EPSILON) * gain_ref[...]
        rows = pl.ds(b * block, block)
        h_next[rows] = (h_next[rows].astype(F32) + normed).astype(BF16)
        return carry

    def received(step, base, count):
        return recv[step, pl.ds(base, count)].reshape(count * slot, width)

    h_next[...] = h_ref[...]
    pass_on(0)
    pass_on(1)
    swap_copy(0).wait_recv()
    swap_copy(1).wait_recv()
    lax.fori_loop(0, blocks, project, 0)
    lax.fori_loop(0, blocks, local_edges, 0)
    for i in range(2, pieces):
        pass_on(i)
    for i in range(2, pieces):
        swap_copy(i).wait_recv()
    lax.fori_loop(0, blocks, node_part, 0)

    scale = None
    for step in range(STEPS):
        if step > 0:
            scale = finish_sum(step - 1)
            cons_ref[step - 1] = scale * local_fields
            mix = (scale - 1.0) * we_ref[...]

            def move(b, carry):
                rows = pl.ds(b * block, block)
                h_next[rows] = rescaled(h_next[rows], mix)
                return carry

            lax.fori_loop(0, blocks, move, 0)
            lax.fori_loop(0, blocks, project, 0)
            lax.fori_loop(0, blocks, local_edges, 0)
            lax.fori_loop(0, blocks, node_part, 0)

        def place_rows(base):
            rows = received(step, base, half)
            if step > 0:
                rows = rescaled(rows, mix)
            table[pl.ds(nodes + base * slot, fan)] = (0.5 * mm(rows, w[0])).astype(BF16)

        wait_far(step)
        place_rows(half)
        lax.fori_loop(0, blocks * deg, far_edges, 0)
        wait_near(step)
        place_rows(0)
        lax.fori_loop(0, blocks, finish_block, 0)

        if step + 1 < STEPS:
            fill_send(step + 1, h_next[...])
        local_fields = softplus(lax.dot_general(wd, h_next[...], NT, preferred_element_type=F32))
        start_sum(step, local_fields)
        if step + 1 < STEPS:
            start_exchange(step + 1)

    scale = finish_sum(STEPS - 1)
    cons_ref[STEPS - 1] = scale * local_fields
    mix = (scale - 1.0) * we_ref[...]

    def leave(b, carry):
        rows = pl.ds(b * block, block)
        out_ref[rows] = rescaled(h_next[rows], mix)
        return carry

    lax.fori_loop(0, blocks, leave, 0)

    for i in range(pieces):
        for offset in range(1, n_feat):
            shard_copy(i, offset).wait_send()
        swap_copy(i).wait_send()
    for step in range(STEPS):
        ref = send.at[step, pl.ds(0, n_patch - 1)]
        pltpu.make_async_copy(ref, ref, as_sem.at[step]).wait()
        ref = ar_all.at[step, pl.ds(0, n_patch - 1)]
        pltpu.make_async_copy(ref, ref, ps_sem.at[step]).wait()
        for offset in range(1, n_feat):
            side_copy(step, offset).wait_send()


def shards(
    n_patch,
    n_feat,
    latents,
    neighbours,
    degree,
    send_rows,
    area,
    scenario,
    totals,
    w_send,
    w_recv,
    b_edge,
    w_msg,
    w_node,
    w_out,
    gain,
    w_dec,
    w_enc,
):
    nodes, width = latents.shape
    deg, slot = neighbours.shape[1], send_rows.shape[1]
    fields = w_dec.shape[0]
    block = min(256, nodes)
    blocks = nodes // block
    fan = n_patch // 2 * slot
    pieces = 6
    lanes = 128
    vmem = pl.BlockSpec(memory_space=pltpu.VMEM)
    hbm = pl.BlockSpec(memory_space=pltpu.HBM)
    dma = pltpu.SemaphoreType.DMA
    return pl.pallas_call(
        functools.partial(kernel, n_patch, n_feat),
        out_shape=(
            jax.ShapeDtypeStruct((nodes, width), BF16),
            jax.ShapeDtypeStruct((STEPS, fields, nodes), F32),
        ),
        in_specs=[vmem] * 7 + [hbm, hbm, vmem, hbm, hbm, hbm, vmem, vmem, vmem],
        out_specs=(vmem, vmem),
        scratch_shapes=[
            pltpu.VMEM((pieces, width, width), BF16),
            pltpu.VMEM((nodes, deg), jnp.int32),
            pltpu.VMEM((n_patch * slot, nodes), BF16),
            pltpu.VMEM((blocks * deg, block, nodes), BF16),
            pltpu.VMEM((blocks * deg, block, fan), BF16),
            pltpu.VMEM((blocks * deg, block, fan), BF16),
            pltpu.VMEM((blocks * deg, block, width), F32),
            pltpu.VMEM((blocks, block, width), F32),
            pltpu.VMEM((nodes + 2 * fan, width), BF16),
            pltpu.VMEM((blocks, block, width), F32),
            pltpu.VMEM((blocks, block, width), F32),
            pltpu.VMEM((nodes, width), BF16),
            pltpu.VMEM((STEPS, n_patch, slot, width), BF16),
            pltpu.VMEM((STEPS, n_patch, slot, width), BF16),
            pltpu.VMEM((STEPS, 1, lanes), F32),
            pltpu.VMEM((STEPS, n_patch, 1, lanes), F32),
            pltpu.VMEM((STEPS, 1, lanes), F32),
            pltpu.VMEM((STEPS, n_feat, 1, lanes), F32),
            dma((pieces,)),
            dma((pieces, n_feat - 1)),
            dma((pieces, n_feat - 1)),
            dma((pieces,)),
            dma((pieces,)),
            dma((STEPS,)),
            dma((STEPS, 2)),
            dma((STEPS,)),
            dma((STEPS,)),
            dma((STEPS, n_feat - 1)),
            dma((STEPS, n_feat - 1)),
        ],
        compiler_params=pltpu.CompilerParams(
            collective_id=0, has_side_effects=True, vmem_limit_bytes=63 * 1024 * 1024
        ),
    )(
        latents,
        neighbours.T,
        degree[None, :],
        send_rows.T,
        area[None, :],
        scenario[None, :],
        totals,
        w_send,
        w_recv,
        b_edge,
        w_msg,
        w_node,
        w_out,
        gain,
        w_dec,
        w_enc,
    )


def solution(mesh):
    every = ("members", "patch", "feat")
    group = ("patch", "feat")
    column = P(None, None, "feat")
    return jax.shard_map(
        functools.partial(shards, mesh.shape["patch"], mesh.shape["feat"]),
        mesh=mesh,
        in_specs=(
            P(every, None),
            P(group, None),
            P(group),
            P(group, None),
            P(group),
            P("members"),
            P(),
            column,
            column,
            P(),
            column,
            column,
            column,
            P(),
            P(),
            P(),
        ),
        out_specs=(P(every, None), P("members", None, group)),
        check_vma=False,
    )
```

```python
import functools

import jax
import jax.numpy as jnp
from jax import lax
from jax.experimental import pallas as pl
from jax.experimental.pallas import tpu as pltpu
from jax.sharding import PartitionSpec as P

STEPS = 2
EPSILON = 1e-05
DEAD = -1e30
MESH = pl.DeviceIdType.MESH
F32 = jnp.float32
BF16 = jnp.bfloat16
NT = (((1,), (1,)), ((), ()))


def mm(a, b):
    return jnp.dot(a, b, preferred_element_type=F32)


def half_silu(half):
    return half * jnp.tanh(half) + half


def softplus(x):
    return jnp.maximum(x, 0.0) + jnp.log1p(jnp.exp(-jnp.abs(x)))


def kernel(
    n_patch,
    n_feat,
    h_ref,
    nbr_ref,
    deg_ref,
    rows_ref,
    area_ref,
    scen_ref,
    tot_ref,
    ws_ref,
    wr_ref,
    be_ref,
    wm_ref,
    wn_ref,
    wo_ref,
    gain_ref,
    wd_ref,
    we_ref,
    out_ref,
    cons_ref,
    w,
    ids,
    ohs,
    ohl,
    ohr,
    pre,
    table,
    recv_half,
    h_node,
    h_next,
    summed,
    send,
    recv,
    ar_src,
    ar_all,
    ax_src,
    ax_all,
    in_sem,
    token_sem,
    h_sem,
    wl_sem,
    ws_sem,
    wr_sem,
    fs_sem,
    fr_sem,
    as_sem,
    ar_sem,
    ps_sem,
    pr_sem,
    xs_sem,
    xr_sem,
):
    nodes, width = h_ref.shape
    deg = nbr_ref.shape[0]
    slot = rows_ref.shape[0]
    groups, packed = pre.shape[0], pre.shape[1]
    few = packed // deg
    blocks, block = h_node.shape[0], h_node.shape[1]
    cols = ws_ref.shape[2]
    half = n_patch // 2
    parts = ar_sem.shape[1]
    part_slots = n_patch // parts
    remote = n_patch * slot
    pieces = w.shape[0]
    unroll = 4 if groups % 4 == 0 else 1
    me = lax.axis_index("patch")
    feat = lax.axis_index("feat")
    core = lax.rem(me, 2)
    partner = me + 1 - 2 * core

    def peer(offset):
        return lax.rem(me + offset, n_patch)

    def side(offset):
        return lax.rem(feat + offset, n_feat)

    rank = lax.rem(me + n_patch - 1, n_patch)
    ahead = peer(1)
    behind = peer(n_patch - 1)
    barrier = pltpu.get_barrier_semaphore()
    pl.semaphore_signal(barrier, inc=1, device_id={"patch": behind}, device_id_type=MESH)
    for offset in range(1, n_feat):
        pl.semaphore_signal(barrier, inc=1, device_id={"feat": side(offset)}, device_id_type=MESH)

    span = width // 2
    mine = pl.ds(pl.multiple_of(core * span, span), span)
    low = mine
    high = pl.ds(pl.multiple_of(width + core * span, span), span)
    shards = (
        ws_ref.at[0, low],
        wr_ref.at[0, low],
        wn_ref.at[0, low],
        wm_ref.at[0, low],
        wn_ref.at[0, high],
        wo_ref.at[0, low],
    )

    def cols_of(owner):
        return pl.ds(pl.multiple_of(owner * cols, cols), cols)

    own_cols = cols_of(feat)
    load_h = pltpu.make_async_copy(h_ref, h_next, h_sem)
    local = [
        pltpu.make_async_copy(shards[i], w.at[i, mine, own_cols], wl_sem.at[i])
        for i in range(pieces)
    ]
    local[0].start()
    local[1].start()
    load_h.start()
    for i in range(2, pieces):
        local[i].start()

    pl.semaphore_wait(barrier, n_feat)

    @pl.when(rank > 0)
    def _():
        pl.semaphore_wait(token_sem, 1)

    @pl.when(rank < n_patch - 1)
    def _():
        pl.semaphore_signal(token_sem, inc=1, device_id={"patch": ahead}, device_id_type=MESH)

    def arrive(back, carry):
        pl.semaphore_signal(
            in_sem.at[rank],
            inc=1,
            device_id={"patch": peer(n_patch - back)},
            device_id_type=MESH,
        )
        return carry

    lax.fori_loop(1, rank + 1, arrive, 0)

    def side_part(i, rows, owner, to, at):
        ref = w.at[i, rows, cols_of(owner)]
        return pltpu.make_async_remote_copy(
            src_ref=ref,
            dst_ref=ref,
            send_sem=ws_sem.at[i, at],
            recv_sem=wr_sem.at[i, at],
            device_id={"feat": to},
            device_id_type=MESH,
        )

    right, left = side(1), side(n_feat - 1)
    relay = n_feat == 4
    quart = span // 2
    rows_a = pl.ds(pl.multiple_of(core * span, quart), quart)
    rows_b = pl.ds(pl.multiple_of(core * span + quart, quart), quart)

    def first_copies(i):
        if relay:
            return [side_part(i, mine, feat, right, 0), side_part(i, mine, feat, left, 1)]
        return [side_part(i, mine, feat, side(o), o - 1) for o in range(1, n_feat)]

    def relay_copies(i):
        if relay:
            return [side_part(i, rows_a, left, right, 2), side_part(i, rows_b, right, left, 3)]
        return []

    def swap_copy(i):
        return pltpu.make_async_remote_copy(
            src_ref=w.at[i, mine],
            dst_ref=w.at[i, mine],
            send_sem=fs_sem.at[i],
            recv_sem=fr_sem.at[i],
            device_id={"patch": partner},
            device_id_type=MESH,
        )

    def own_out(i):
        local[i].wait()
        for copy in first_copies(i):
            copy.start()

    def pass_on(i):
        for copy in first_copies(i):
            copy.wait_recv()
        for copy in relay_copies(i):
            copy.start()

    def pass_over(i):
        for copy in relay_copies(i):
            copy.wait_recv()
        swap_copy(i).start()

    own_out(0)
    own_out(1)

    picks = rows_ref[...].T.astype(F32)
    spread = jnp.where(
        lax.broadcasted_iota(jnp.int32, (remote, n_patch), 0) // slot
        == lax.broadcasted_iota(jnp.int32, (remote, n_patch), 1),
        1.0,
        0.0,
    ).astype(BF16)
    coarse = jnp.floor(picks * (1.0 / 16.0))
    fine = picks - 16.0 * coarse
    each = mm(spread, coarse.astype(BF16)) * 16.0 + mm(spread, fine.astype(BF16))
    lane = lax.broadcasted_iota(jnp.int32, (remote, slot), 1)
    turn = lax.broadcasted_iota(jnp.int32, (remote, slot), 0) % slot
    chosen_row = jnp.sum(jnp.where(lane == turn, each, 0.0), axis=1, keepdims=True)
    node_at = lax.broadcasted_iota(jnp.int32, (remote, nodes), 1).astype(F32)
    ohs[...] = jnp.where(chosen_row == node_at, 1.0, 0.0).astype(BF16)

    def fill_send(step):
        picked = mm(ohs[...], h_next[...]).astype(BF16).reshape(n_patch, slot, width)
        send[step] = picked
        recv[step, pl.ds(n_patch - 1, 1)] = send[step, pl.ds(me, 1)]

    load_h.wait()
    fill_send(0)

    def slot_of(d):
        return jnp.where(d < 0, -2 * d - 1, 2 * d)

    def exchange(step, offset):
        target = peer(offset)
        place = slot_of(half - offset)
        pltpu.make_async_remote_copy(
            src_ref=send.at[step, target],
            dst_ref=recv.at[step, place],
            send_sem=as_sem.at[step],
            recv_sem=ar_sem.at[step, place // part_slots],
            device_id={"patch": target},
            device_id_type=MESH,
        ).start()

    def exchange_pairs(step, first, last):
        def body(j, carry):
            exchange(step, half - j)
            exchange(step, half + j)
            return carry

        if first == 0:
            exchange(step, half)
        lax.fori_loop(max(first, 1), last, body, 0)

    def wait_part(step, g):
        count = part_slots - 1 if g == parts - 1 else part_slots
        ref = recv.at[step, pl.ds(0, count)]
        pltpu.make_async_copy(ref, ref, ar_sem.at[step, g]).wait()

    def send_back(back, carry):
        exchange(0, n_patch - back)
        return carry

    def send_ahead(on, carry):
        pl.semaphore_wait(in_sem.at[rank + on], 1)
        exchange(0, on)
        return carry

    lax.fori_loop(1, rank + 1, send_back, 0)
    pass_on(0)
    pass_on(1)
    for i in range(2, pieces):
        own_out(i)
    lax.fori_loop(1, n_patch - rank, send_ahead, 0)

    raw = nbr_ref[...]
    far_id = jnp.maximum(raw - nodes, 0)
    source = far_id // slot - me
    source = jnp.where(source < 0, source + n_patch, source)
    ordered = jnp.where(raw < nodes, raw, nodes + slot_of(source - half) * slot + far_id % slot)
    live = lax.broadcasted_iota(jnp.int32, raw.shape, 0) < deg_ref[...].reshape(1, nodes)
    ids[...] = jnp.where(live, ordered, -1).T

    def select(g, carry):
        mine_ids = ids[pl.ds(g * few, few)]
        for k in range(deg):
            col = mine_ids[:, k : k + 1]
            for ref, base in ((ohl, 0), (ohr, nodes)):
                here = lax.broadcasted_iota(jnp.int32, (few, ref.shape[2]), 1) + base
                ref[g, pl.ds(k * few, few)] = jnp.where(col == here, 1.0, 0.0).astype(BF16)
        return carry

    lax.fori_loop(0, groups, select, 0)

    fields = wd_ref.shape[0]
    nodes_all = float(nodes * n_patch * n_feat)
    field_at = lax.broadcasted_iota(jnp.int32, tot_ref.shape, 0)
    wanted = jnp.zeros(tot_ref.shape, jnp.int32)
    for f in range(fields):
        wanted = jnp.where(field_at == f, scen_ref[f], wanted)
    scenario_at = lax.broadcasted_iota(jnp.int32, tot_ref.shape, 1)
    target = jnp.sum(jnp.where(scenario_at == wanted, tot_ref[...], 0.0), axis=1, keepdims=True)
    lanes = ar_src.shape[2]
    mark = lax.broadcasted_iota(jnp.int32, (fields, lanes), 0) == lax.broadcasted_iota(
        jnp.int32, (fields, lanes), 1
    )
    plane = 2 * n_feat
    seat = core * n_feat + feat
    depth = lax.div(me, 2)

    def seat_copy(step, offset):
        other = lax.rem(seat + offset, plane)
        other_core = lax.div(other, n_feat)
        return pltpu.make_async_remote_copy(
            src_ref=ax_src.at[step],
            dst_ref=ax_all.at[step, seat],
            send_sem=xs_sem.at[step],
            recv_sem=xr_sem.at[step],
            device_id={"patch": me - core + other_core, "feat": lax.rem(other, n_feat)},
            device_id_type=MESH,
        )

    def wait_bytes(ref, sem):
        pltpu.make_async_copy(ref, ref, sem).wait()

    def start_sum(step, local_fields):
        area = area_ref[...].reshape(1, nodes)
        part = jnp.sum(local_fields * area, axis=1, keepdims=True)
        wide = jnp.broadcast_to(part, (fields, lanes))
        line = jnp.sum(jnp.where(mark, wide, 0.0), axis=0, keepdims=True)
        ax_src[step] = line
        ax_all[step, pl.ds(seat, 1)] = line.reshape(1, 1, lanes)
        for offset in range(1, plane):
            seat_copy(step, offset).start()
        wait_bytes(ax_all.at[step, pl.ds(0, plane - 1)], xr_sem.at[step])
        line = jnp.sum(ax_all[step], axis=0)
        ar_src[step] = line
        ar_all[step, pl.ds(depth, 1)] = line.reshape(1, 1, lanes)

        def one(offset):
            pltpu.make_async_remote_copy(
                src_ref=ar_src.at[step],
                dst_ref=ar_all.at[step, depth],
                send_sem=ps_sem.at[step],
                recv_sem=pr_sem.at[step],
                device_id={"patch": peer(2 * offset)},
                device_id_type=MESH,
            ).start()

        middle = half // 2

        def both(j, carry):
            one(middle - j)
            one(middle + j)
            return carry

        one(middle)
        lax.fori_loop(1, middle, both, 0)

    def finish_sum(step):
        wait_bytes(ar_all.at[step, pl.ds(0, half - 1)], pr_sem.at[step])
        line = jnp.sum(ar_all[step], axis=0)
        wide = jnp.broadcast_to(line, (fields, lanes))
        integral = jnp.sum(jnp.where(mark, wide, 0.0), axis=1, keepdims=True)
        return target * nodes_all / integral

    wd = wd_ref[...]

    def rescaled(rows, mix):
        part = softplus(lax.dot_general(rows, wd, NT, preferred_element_type=F32))
        change = jnp.dot(part, mix, precision=lax.Precision.HIGHEST, preferred_element_type=F32)
        return (rows.astype(F32) + change).astype(BF16)

    def project(b, carry):
        rows = pl.ds(b * block, block)
        latent = h_next[rows]
        table[rows] = (0.5 * mm(latent, w[0])).astype(BF16)
        recv_half[rows] = 0.5 * (mm(latent, w[1]) + be_ref[...])
        return carry

    def local_edges(t, carry):
        for u in range(unroll):
            g = t * unroll + u
            here = pl.ds(g * few, few)
            mine_ids = ids[here]
            base = recv_half[here]
            found = mm(ohl[g], table[pl.ds(0, nodes)])
            for k in range(deg):
                dead = jnp.where(mine_ids[:, k : k + 1] < 0, DEAD, 0.0)
                pre[g, pl.ds(k * few, few)] = found[k * few : (k + 1) * few] + (base + dead)
        return carry

    def node_part(b, carry):
        h_node[b] = mm(h_next[pl.ds(b * block, block)], w[2])
        return carry

    def remote_edges(t, carry):
        for u in range(unroll):
            g = t * unroll + u
            found = mm(ohr[g], table[pl.ds(nodes, remote)])
            total = jnp.zeros((few, width), F32)
            for k in range(deg):
                rows = pl.ds(k * few, few)
                total = total + half_silu(pre[g, rows] + found[k * few : (k + 1) * few])
            summed[pl.ds(g * few, few)] = total.astype(BF16)
        return carry

    def finish_block(b):
        rows = pl.ds(b * block, block)
        message = mm(summed[rows], w[3]).astype(BF16)
        hidden = half_silu(0.5 * (h_node[b] + mm(message, w[4]))).astype(BF16)
        output = mm(hidden, w[5])
        average = jnp.mean(output, axis=1, keepdims=True)
        centred = output - average
        variance = jnp.mean(jnp.square(centred), axis=1, keepdims=True)
        normed = centred * lax.rsqrt(variance + EPSILON) * gain_ref[...]
        h_next[rows] = (h_next[rows].astype(F32) + normed).astype(BF16)

    def place_part(step, g, mix):
        rows = recv[step, pl.ds(g * part_slots, part_slots)]
        rows = rows.reshape(part_slots * slot, width)
        if step > 0:
            rows = rescaled(rows, mix)
        at = pl.ds(nodes + g * part_slots * slot, part_slots * slot)
        table[at] = (0.5 * mm(rows, w[0])).astype(BF16)

    pass_over(0)
    pass_over(1)
    swap_copy(0).wait_recv()
    swap_copy(1).wait_recv()
    lax.fori_loop(0, blocks, project, 0)
    for i in range(2, pieces):
        pass_on(i)
    lax.fori_loop(0, groups // unroll, local_edges, 0)
    for i in range(2, pieces):
        pass_over(i)

    mix = None
    for step in range(STEPS):
        if step > 0:
            scale = finish_sum(step - 1)
            for f in range(fields):
                cons_ref[f, step - 1 : step] = (scale * local_fields)[f : f + 1]
            mix = (scale - 1.0) * we_ref[...]

            def move(b, carry):
                rows = pl.ds(b * block, block)
                h_next[rows] = rescaled(h_next[rows], mix)
                return carry

            lax.fori_loop(0, blocks, move, 0)
            lax.fori_loop(0, blocks, project, 0)
            lax.fori_loop(0, groups // unroll, local_edges, 0)
            lax.fori_loop(0, blocks, node_part, 0)

        for g in range(parts):
            wait_part(step, g)
            place_part(step, g, mix)
        lax.fori_loop(0, groups // unroll, remote_edges, 0)
        if step == 0:
            for i in range(2, pieces):
                swap_copy(i).wait_recv()
            lax.fori_loop(0, blocks, node_part, 0)
        for b in range(blocks):
            finish_block(b)

        if step + 1 < STEPS:
            fill_send(step + 1)
            early = half // 4
            exchange_pairs(step + 1, 0, early)
        local_fields = softplus(lax.dot_general(wd, h_next[...], NT, preferred_element_type=F32))
        start_sum(step, local_fields)
        if step + 1 < STEPS:
            exchange_pairs(step + 1, early, half)

    scale = finish_sum(STEPS - 1)
    for f in range(fields):
        cons_ref[f, STEPS - 1 : STEPS] = (scale * local_fields)[f : f + 1]
    mix = (scale - 1.0) * we_ref[...]

    def leave(b, carry):
        rows = pl.ds(b * block, block)
        out_ref[rows] = rescaled(h_next[rows], mix)
        return carry

    lax.fori_loop(0, blocks, leave, 0)

    for i in range(pieces):
        for copy in first_copies(i) + relay_copies(i):
            copy.wait_send()
        swap_copy(i).wait_send()
    for step in range(STEPS):
        wait_bytes(send.at[step, pl.ds(0, n_patch - 1)], as_sem.at[step])
        wait_bytes(ar_all.at[step, pl.ds(0, half - 1)], ps_sem.at[step])
        wait_bytes(ax_all.at[step, pl.ds(0, plane - 1)], xs_sem.at[step])


def shards(
    n_patch,
    n_feat,
    latents,
    neighbours,
    degree,
    send_rows,
    area,
    scenario,
    totals,
    w_send,
    w_recv,
    b_edge,
    w_msg,
    w_node,
    w_out,
    gain,
    w_dec,
    w_enc,
):
    nodes, width = latents.shape
    deg, slot = neighbours.shape[1], send_rows.shape[1]
    fields = w_dec.shape[0]
    block = min(256, nodes)
    blocks = nodes // block
    few = 32
    groups = nodes // few
    remote = n_patch * slot
    pieces = 6
    parts = 4
    lanes = 128
    sides = max(n_feat, 2)
    vmem = pl.BlockSpec(memory_space=pltpu.VMEM)
    smem = pl.BlockSpec(memory_space=pltpu.SMEM)
    hbm = pl.BlockSpec(memory_space=pltpu.HBM)
    dma = pltpu.SemaphoreType.DMA
    final, conserved = pl.pallas_call(
        functools.partial(kernel, n_patch, n_feat),
        out_shape=(
            jax.ShapeDtypeStruct((nodes, width), BF16),
            jax.ShapeDtypeStruct((fields, STEPS, nodes), F32),
        ),
        in_specs=[hbm, vmem, vmem, vmem, vmem, smem, vmem, hbm, hbm, vmem, hbm, hbm, hbm]
        + [vmem] * 3,
        out_specs=(vmem, vmem),
        scratch_shapes=[
            pltpu.VMEM((pieces, width, width), BF16),
            pltpu.VMEM((nodes, deg), jnp.int32),
            pltpu.VMEM((remote, nodes), BF16),
            pltpu.VMEM((groups, deg * few, nodes), BF16),
            pltpu.VMEM((groups, deg * few, remote), BF16),
            pltpu.VMEM((groups, deg * few, width), F32),
            pltpu.VMEM((nodes + remote, width), BF16),
            pltpu.VMEM((nodes, width), F32),
            pltpu.VMEM((blocks, block, width), F32),
            pltpu.VMEM((nodes, width), BF16),
            pltpu.VMEM((nodes, width), BF16),
            pltpu.VMEM((STEPS, n_patch, slot, width), BF16),
            pltpu.VMEM((STEPS, n_patch, slot, width), BF16),
            pltpu.VMEM((STEPS, 1, lanes), F32),
            pltpu.VMEM((STEPS, n_patch // 2, 1, lanes), F32),
            pltpu.VMEM((STEPS, 1, lanes), F32),
            pltpu.VMEM((STEPS, 2 * n_feat, 1, lanes), F32),
            pltpu.SemaphoreType.REGULAR((n_patch,)),
            pltpu.SemaphoreType.REGULAR,
            dma,
            dma((pieces,)),
            dma((pieces, sides)),
            dma((pieces, sides)),
            dma((pieces,)),
            dma((pieces,)),
            dma((STEPS,)),
            dma((STEPS, parts)),
            dma((STEPS,)),
            dma((STEPS,)),
            dma((STEPS,)),
            dma((STEPS,)),
        ],
        compiler_params=pltpu.CompilerParams(
            collective_id=0, has_side_effects=True, vmem_limit_bytes=63 * 1024 * 1024
        ),
    )(
        latents,
        neighbours.T,
        degree,
        send_rows.T,
        area,
        scenario,
        totals.T,
        w_send,
        w_recv,
        b_edge,
        w_msg,
        w_node,
        w_out,
        gain,
        w_dec,
        w_enc,
    )
    return final, jnp.transpose(conserved, (1, 0, 2))


def solution(mesh):
    every = ("members", "patch", "feat")
    group = ("patch", "feat")
    column = P(None, None, "feat")
    return jax.shard_map(
        functools.partial(shards, mesh.shape["patch"], mesh.shape["feat"]),
        mesh=mesh,
        in_specs=(
            P(every, None),
            P(group, None),
            P(group),
            P(group, None),
            P(group),
            P("members"),
            P(),
            column,
            column,
            P(),
            column,
            column,
            column,
            P(),
            P(),
            P(),
        ),
        out_specs=(P(every, None), P("members", None, group)),
        check_vma=False,
    )
```

```python
import functools

import jax
import jax.numpy as jnp
from jax import lax
from jax.experimental import pallas as pl
from jax.experimental.pallas import tpu as pltpu
from jax.sharding import PartitionSpec as P

STEPS = 2
EPSILON = 1e-05
DEAD = -1e30
MESH = pl.DeviceIdType.MESH
F32 = jnp.float32
BF16 = jnp.bfloat16
NT = (((1,), (1,)), ((), ()))


def mm(a, b):
    return jnp.dot(a, b, preferred_element_type=F32)


def half_silu(half):
    return half * jnp.tanh(half) + half


def softplus(x):
    return jnp.maximum(x, 0.0) + jnp.log1p(jnp.exp(-jnp.abs(x)))


def kernel(
    n_patch,
    n_feat,
    h_ref,
    nbr_ref,
    deg_ref,
    rows_ref,
    area_ref,
    scen_ref,
    tot_ref,
    ws_ref,
    wr_ref,
    be_ref,
    wm_ref,
    wn_ref,
    wo_ref,
    gain_ref,
    wd_ref,
    we_ref,
    out_ref,
    change_ref,
    cons_ref,
    w,
    ids,
    ohs,
    ohl,
    ohr,
    pre,
    table,
    recv_half,
    h_node,
    h_next,
    summed,
    send,
    recv,
    ar_src,
    ar_all,
    ax_src,
    ax_all,
    in_sem,
    token_sem,
    pair_sem,
    h_sem,
    out_sem,
    wl_sem,
    ws_sem,
    wr_sem,
    fs_sem,
    fr_sem,
    as_sem,
    ar_sem,
    ps_sem,
    pr_sem,
    xs_sem,
    xr_sem,
):
    nodes, width = h_ref.shape
    deg = nbr_ref.shape[0]
    slot = rows_ref.shape[0]
    groups, packed = pre.shape[0], pre.shape[1]
    few = packed // deg
    blocks, block = h_node.shape[0], h_node.shape[1]
    cols = ws_ref.shape[2]
    parts = ar_sem.shape[1]
    part_slots = n_patch // parts
    remote = n_patch * slot
    pieces = w.shape[0]
    unroll = 4 if groups % 4 == 0 else 1
    me = lax.axis_index("patch")
    feat = lax.axis_index("feat")
    core = lax.rem(me, 2)
    partner = me + 1 - 2 * core

    def peer(offset):
        return lax.rem(me + offset, n_patch)

    def side(offset):
        return lax.rem(feat + offset, n_feat)

    rank = lax.rem(me + n_patch - 1, n_patch)
    half = n_patch // 2
    depth = lax.div(me, 2)
    ahead = peer(2)
    behind = peer(n_patch - 2)
    first = jnp.where(core == 1, 0, 1)
    last = jnp.where(core == 1, half - 1, 0)
    paired = depth > 0
    barrier = pltpu.get_barrier_semaphore()

    def greet(**device):
        pl.semaphore_signal(barrier, inc=1, device_id=device, device_id_type=MESH)

    @pl.when(depth != first)
    def _():
        greet(patch=behind)

    @pl.when(paired)
    def _():
        greet(patch=partner)

    for offset in range(1, n_feat):
        greet(feat=side(offset))

    span = width // 2
    mine = pl.ds(pl.multiple_of(core * span, span), span)
    low = mine
    high = pl.ds(pl.multiple_of(width + core * span, span), span)
    shards = (
        ws_ref.at[0, low],
        wr_ref.at[0, low],
        wn_ref.at[0, low],
        wm_ref.at[0, low],
        wn_ref.at[0, high],
        wo_ref.at[0, low],
    )

    def cols_of(owner):
        return pl.ds(pl.multiple_of(owner * cols, cols), cols)

    own_cols = cols_of(feat)
    load_h = pltpu.make_async_copy(h_ref, h_next, h_sem)
    local = [
        pltpu.make_async_copy(shards[i], w.at[i, mine, own_cols], wl_sem.at[i])
        for i in range(pieces)
    ]
    local[0].start()
    local[1].start()
    load_h.start()
    for i in range(2, pieces):
        local[i].start()

    greetings = n_feat - 1 + jnp.where(depth != last, 1, 0) + jnp.where(paired, 1, 0)
    pl.semaphore_wait(barrier, greetings)
    closing = me == n_patch - 2

    def tell_ahead():
        pl.semaphore_signal(token_sem, inc=1, device_id={"patch": ahead}, device_id_type=MESH)

    @pl.when(depth != first)
    def _():
        pl.semaphore_wait(token_sem, 1)

    @pl.when(jnp.logical_and(depth != last, jnp.logical_not(closing)))
    def _():
        tell_ahead()

    @pl.when(paired)
    def _():
        pl.semaphore_signal(pair_sem, inc=1, device_id={"patch": partner}, device_id_type=MESH)
        pl.semaphore_wait(pair_sem, 1)

    @pl.when(closing)
    def _():
        tell_ahead()

    def arrive(back, carry):
        pl.semaphore_signal(
            in_sem.at[rank],
            inc=1,
            device_id={"patch": peer(n_patch - back)},
            device_id_type=MESH,
        )
        return carry

    lax.fori_loop(1, rank + 1, arrive, 0)

    def side_part(i, rows, owner, to, at):
        ref = w.at[i, rows, cols_of(owner)]
        return pltpu.make_async_remote_copy(
            src_ref=ref,
            dst_ref=ref,
            send_sem=ws_sem.at[i, at],
            recv_sem=wr_sem.at[i, at],
            device_id={"feat": to},
            device_id_type=MESH,
        )

    right, left = side(1), side(n_feat - 1)
    relay = n_feat == 4
    quart = span // 2
    rows_a = pl.ds(pl.multiple_of(core * span, quart), quart)
    rows_b = pl.ds(pl.multiple_of(core * span + quart, quart), quart)

    def first_copies(i):
        if relay:
            return [side_part(i, mine, feat, right, 0), side_part(i, mine, feat, left, 1)]
        return [side_part(i, mine, feat, side(o), o - 1) for o in range(1, n_feat)]

    def relay_copies(i):
        if relay:
            return [side_part(i, rows_a, left, right, 2), side_part(i, rows_b, right, left, 3)]
        return []

    def swap_copy(i):
        return pltpu.make_async_remote_copy(
            src_ref=w.at[i, mine],
            dst_ref=w.at[i, mine],
            send_sem=fs_sem.at[i],
            recv_sem=fr_sem.at[i],
            device_id={"patch": partner},
            device_id_type=MESH,
        )

    def own_out(i):
        local[i].wait()
        for copy in first_copies(i):
            copy.start()

    def pass_on(i):
        for copy in first_copies(i):
            copy.wait_recv()
        for copy in relay_copies(i):
            copy.start()

    def pass_over(i):
        for copy in relay_copies(i):
            copy.wait_recv()
        swap_copy(i).start()

    own_out(0)
    own_out(1)

    picks = rows_ref[...].T.astype(F32)
    spread = jnp.where(
        lax.broadcasted_iota(jnp.int32, (remote, n_patch), 0) // slot
        == lax.broadcasted_iota(jnp.int32, (remote, n_patch), 1),
        1.0,
        0.0,
    ).astype(BF16)
    coarse = jnp.floor(picks * (1.0 / 16.0))
    fine = picks - 16.0 * coarse
    each = mm(spread, coarse.astype(BF16)) * 16.0 + mm(spread, fine.astype(BF16))
    lane = lax.broadcasted_iota(jnp.int32, (remote, slot), 1)
    turn = lax.broadcasted_iota(jnp.int32, (remote, slot), 0) % slot
    chosen_row = jnp.sum(jnp.where(lane == turn, each, 0.0), axis=1, keepdims=True)
    node_at = lax.broadcasted_iota(jnp.int32, (remote, nodes), 1).astype(F32)
    ohs[...] = jnp.where(chosen_row == node_at, 1.0, 0.0).astype(BF16)

    def fill_send(step):
        picked = mm(ohs[...], h_next[...]).astype(BF16).reshape(n_patch, slot, width)
        send[step] = picked
        recv[step, pl.ds(n_patch - 1, 1)] = send[step, pl.ds(me, 1)]

    load_h.wait()
    fill_send(0)

    def slot_of(d):
        return jnp.where(d < 0, -2 * d - 1, 2 * d)

    def exchange(step, offset):
        target = peer(offset)
        place = slot_of(half - offset)
        pltpu.make_async_remote_copy(
            src_ref=send.at[step, target],
            dst_ref=recv.at[step, place],
            send_sem=as_sem.at[step],
            recv_sem=ar_sem.at[step, place // part_slots],
            device_id={"patch": target},
            device_id_type=MESH,
        ).start()

    def exchange_all(step):
        def body(j, carry):
            exchange(step, half - j)
            exchange(step, half + j)
            return carry

        exchange(step, half)
        lax.fori_loop(1, half, body, 0)

    def wait_part(step, g):
        count = part_slots - 1 if g == parts - 1 else part_slots
        ref = recv.at[step, pl.ds(0, count)]
        pltpu.make_async_copy(ref, ref, ar_sem.at[step, g]).wait()

    def send_back(back, carry):
        exchange(0, n_patch - back)
        return carry

    def send_ahead(on, carry):
        pl.semaphore_wait(in_sem.at[rank + on], 1)
        exchange(0, on)
        return carry

    lax.fori_loop(1, rank + 1, send_back, 0)
    pass_on(0)
    pass_on(1)
    for i in range(2, pieces):
        own_out(i)
    lax.fori_loop(1, n_patch - rank, send_ahead, 0)

    raw = nbr_ref[...]
    far_id = jnp.maximum(raw - nodes, 0)
    source = far_id // slot - me
    source = jnp.where(source < 0, source + n_patch, source)
    ordered = jnp.where(raw < nodes, raw, nodes + slot_of(source - half) * slot + far_id % slot)
    live = lax.broadcasted_iota(jnp.int32, raw.shape, 0) < deg_ref[...].reshape(1, nodes)
    ids[...] = jnp.where(live, ordered, -1).T

    def select(g, carry):
        mine_ids = ids[pl.ds(g * few, few)]
        for k in range(deg):
            col = mine_ids[:, k : k + 1]
            for ref, base in ((ohl, 0), (ohr, nodes)):
                here = lax.broadcasted_iota(jnp.int32, (few, ref.shape[2]), 1) + base
                ref[g, pl.ds(k * few, few)] = jnp.where(col == here, 1.0, 0.0).astype(BF16)
        return carry

    lax.fori_loop(0, groups, select, 0)

    fields = wd_ref.shape[0]
    nodes_all = float(nodes * n_patch * n_feat)
    field_at = lax.broadcasted_iota(jnp.int32, tot_ref.shape, 0)
    wanted = jnp.zeros(tot_ref.shape, jnp.int32)
    for f in range(fields):
        wanted = jnp.where(field_at == f, scen_ref[f], wanted)
    scenario_at = lax.broadcasted_iota(jnp.int32, tot_ref.shape, 1)
    target = jnp.sum(jnp.where(scenario_at == wanted, tot_ref[...], 0.0), axis=1, keepdims=True)
    lanes = ar_src.shape[2]
    mark = lax.broadcasted_iota(jnp.int32, (fields, lanes), 0) == lax.broadcasted_iota(
        jnp.int32, (fields, lanes), 1
    )
    plane = 2 * n_feat
    seat = core * n_feat + feat

    def seat_copy(step, offset):
        other = lax.rem(seat + offset, plane)
        other_core = lax.div(other, n_feat)
        return pltpu.make_async_remote_copy(
            src_ref=ax_src.at[step],
            dst_ref=ax_all.at[step, seat],
            send_sem=xs_sem.at[step],
            recv_sem=xr_sem.at[step],
            device_id={"patch": me - core + other_core, "feat": lax.rem(other, n_feat)},
            device_id_type=MESH,
        )

    def wait_bytes(ref, sem):
        pltpu.make_async_copy(ref, ref, sem).wait()

    def put_sum(step, local_fields):
        area = area_ref[...].reshape(1, nodes)
        part = jnp.sum(local_fields * area, axis=1, keepdims=True)
        wide = jnp.broadcast_to(part, (fields, lanes))
        line = jnp.sum(jnp.where(mark, wide, 0.0), axis=0, keepdims=True)
        ar_src[step] = line
        ar_all[step, pl.ds(depth, 1)] = line.reshape(1, 1, lanes)

    def send_sum(step):
        def one(offset):
            pltpu.make_async_remote_copy(
                src_ref=ar_src.at[step],
                dst_ref=ar_all.at[step, depth],
                send_sem=ps_sem.at[step],
                recv_sem=pr_sem.at[step],
                device_id={"patch": peer(2 * offset)},
                device_id_type=MESH,
            ).start()

        middle = half // 2

        def both(j, carry):
            one(middle - j)
            one(middle + j)
            return carry

        one(middle)
        lax.fori_loop(1, middle, both, 0)

    def finish_sum(step):
        wait_bytes(ar_all.at[step, pl.ds(0, half - 1)], pr_sem.at[step])
        line = jnp.sum(ar_all[step], axis=0)
        ax_src[step] = line
        ax_all[step, pl.ds(seat, 1)] = line.reshape(1, 1, lanes)
        for offset in range(1, plane):
            seat_copy(step, offset).start()
        wait_bytes(ax_all.at[step, pl.ds(0, plane - 1)], xr_sem.at[step])
        line = jnp.sum(ax_all[step], axis=0)
        wide = jnp.broadcast_to(line, (fields, lanes))
        integral = jnp.sum(jnp.where(mark, wide, 0.0), axis=1, keepdims=True)
        return target * nodes_all / integral

    wd = wd_ref[...]

    def rescaled(rows, mix):
        part = softplus(lax.dot_general(rows, wd, NT, preferred_element_type=F32))
        change = jnp.dot(part, mix, precision=lax.Precision.HIGHEST, preferred_element_type=F32)
        return (rows.astype(F32) + change).astype(BF16)

    def project(b, carry):
        rows = pl.ds(b * block, block)
        latent = h_next[rows]
        table[rows] = (0.5 * mm(latent, w[0])).astype(BF16)
        recv_half[rows] = 0.5 * (mm(latent, w[1]) + be_ref[...])
        return carry

    def local_edges(t, carry):
        for u in range(unroll):
            g = t * unroll + u
            here = pl.ds(g * few, few)
            mine_ids = ids[here]
            base = recv_half[here]
            found = mm(ohl[g], table[pl.ds(0, nodes)])
            for k in range(deg):
                dead = jnp.where(mine_ids[:, k : k + 1] < 0, DEAD, 0.0)
                pre[g, pl.ds(k * few, few)] = found[k * few : (k + 1) * few] + (base + dead)
        return carry

    def node_part(b, carry):
        h_node[b] = mm(h_next[pl.ds(b * block, block)], w[2])
        return carry

    def remote_edges(t, carry):
        for u in range(unroll):
            g = t * unroll + u
            found = mm(ohr[g], table[pl.ds(nodes, remote)])
            total = jnp.zeros((few, width), F32)
            for k in range(deg):
                rows = pl.ds(k * few, few)
                total = total + half_silu(pre[g, rows] + found[k * few : (k + 1) * few])
            summed[pl.ds(g * few, few)] = total.astype(BF16)
        return carry

    def finish_block(b):
        rows = pl.ds(b * block, block)
        message = mm(summed[rows], w[3]).astype(BF16)
        hidden = half_silu(0.5 * (h_node[b] + mm(message, w[4]))).astype(BF16)
        output = mm(hidden, w[5])
        average = jnp.mean(output, axis=1, keepdims=True)
        centred = output - average
        variance = jnp.mean(jnp.square(centred), axis=1, keepdims=True)
        normed = centred * lax.rsqrt(variance + EPSILON) * gain_ref[...]
        h_next[rows] = (h_next[rows].astype(F32) + normed).astype(BF16)

    def place_part(step, g, mix):
        rows = recv[step, pl.ds(g * part_slots, part_slots)]
        rows = rows.reshape(part_slots * slot, width)
        if step > 0:
            rows = rescaled(rows, mix)
        at = pl.ds(nodes + g * part_slots * slot, part_slots * slot)
        table[at] = (0.5 * mm(rows, w[0])).astype(BF16)

    pass_over(0)
    pass_over(1)
    swap_copy(0).wait_recv()
    swap_copy(1).wait_recv()
    lax.fori_loop(0, blocks, project, 0)
    for i in range(2, pieces):
        pass_on(i)
    lax.fori_loop(0, groups // unroll, local_edges, 0)
    for i in range(2, pieces):
        pass_over(i)

    mix = None
    for step in range(STEPS):
        if step > 0:
            scale = finish_sum(step - 1)
            for f in range(fields):
                cons_ref[f, step - 1 : step] = (scale * local_fields)[f : f + 1]
            mix = (scale - 1.0) * we_ref[...]

            def move(b, carry):
                rows = pl.ds(b * block, block)
                h_next[rows] = rescaled(h_next[rows], mix)
                return carry

            lax.fori_loop(0, blocks, move, 0)
            lax.fori_loop(0, blocks, project, 0)
            lax.fori_loop(0, groups // unroll, local_edges, 0)
            lax.fori_loop(0, blocks, node_part, 0)

        for g in range(parts):
            wait_part(step, g)
            place_part(step, g, mix)
        lax.fori_loop(0, groups // unroll, remote_edges, 0)
        if step == 0:
            for i in range(2, pieces):
                swap_copy(i).wait_recv()
            lax.fori_loop(0, blocks, node_part, 0)
        for b in range(blocks):
            finish_block(b)

        if step + 1 == STEPS:
            give = pltpu.make_async_copy(h_next, out_ref, out_sem)
            give.start()
        local_fields = softplus(lax.dot_general(wd, h_next[...], NT, preferred_element_type=F32))
        put_sum(step, local_fields)
        if step + 1 < STEPS:
            fill_send(step + 1)
        send_sum(step)
        if step + 1 < STEPS:
            exchange_all(step + 1)

    scale = finish_sum(STEPS - 1)
    change_ref[...] = (scale - 1.0) * local_fields
    for f in range(fields):
        cons_ref[f, STEPS - 1 : STEPS] = (scale * local_fields)[f : f + 1]
    give.wait()

    for i in range(pieces):
        for copy in first_copies(i) + relay_copies(i):
            copy.wait_send()
        swap_copy(i).wait_send()
    for step in range(STEPS):
        wait_bytes(send.at[step, pl.ds(0, n_patch - 1)], as_sem.at[step])
        wait_bytes(ar_all.at[step, pl.ds(0, half - 1)], ps_sem.at[step])
        wait_bytes(ax_all.at[step, pl.ds(0, plane - 1)], xs_sem.at[step])


def shards(
    n_patch,
    n_feat,
    latents,
    neighbours,
    degree,
    send_rows,
    area,
    scenario,
    totals,
    w_send,
    w_recv,
    b_edge,
    w_msg,
    w_node,
    w_out,
    gain,
    w_dec,
    w_enc,
):
    nodes, width = latents.shape
    deg, slot = neighbours.shape[1], send_rows.shape[1]
    fields = w_dec.shape[0]
    block = min(256, nodes)
    blocks = nodes // block
    few = 32
    groups = nodes // few
    remote = n_patch * slot
    pieces = 6
    parts = 4
    lanes = 128
    sides = max(n_feat, 2)
    vmem = pl.BlockSpec(memory_space=pltpu.VMEM)
    smem = pl.BlockSpec(memory_space=pltpu.SMEM)
    hbm = pl.BlockSpec(memory_space=pltpu.HBM)
    dma = pltpu.SemaphoreType.DMA
    latest, change, conserved = pl.pallas_call(
        functools.partial(kernel, n_patch, n_feat),
        out_shape=(
            jax.ShapeDtypeStruct((nodes, width), BF16),
            jax.ShapeDtypeStruct((fields, nodes), F32),
            jax.ShapeDtypeStruct((fields, STEPS, nodes), F32),
        ),
        in_specs=[hbm, vmem, vmem, vmem, vmem, smem, vmem, hbm, hbm, vmem, hbm, hbm, hbm]
        + [vmem] * 3,
        out_specs=(hbm, vmem, vmem),
        scratch_shapes=[
            pltpu.VMEM((pieces, width, width), BF16),
            pltpu.VMEM((nodes, deg), jnp.int32),
            pltpu.VMEM((remote, nodes), BF16),
            pltpu.VMEM((groups, deg * few, nodes), BF16),
            pltpu.VMEM((groups, deg * few, remote), BF16),
            pltpu.VMEM((groups, deg * few, width), F32),
            pltpu.VMEM((nodes + remote, width), BF16),
            pltpu.VMEM((nodes, width), F32),
            pltpu.VMEM((blocks, block, width), F32),
            pltpu.VMEM((nodes, width), BF16),
            pltpu.VMEM((nodes, width), BF16),
            pltpu.VMEM((STEPS, n_patch, slot, width), BF16),
            pltpu.VMEM((STEPS, n_patch, slot, width), BF16),
            pltpu.VMEM((STEPS, 1, lanes), F32),
            pltpu.VMEM((STEPS, n_patch // 2, 1, lanes), F32),
            pltpu.VMEM((STEPS, 1, lanes), F32),
            pltpu.VMEM((STEPS, 2 * n_feat, 1, lanes), F32),
            pltpu.SemaphoreType.REGULAR((n_patch,)),
            pltpu.SemaphoreType.REGULAR,
            pltpu.SemaphoreType.REGULAR,
            dma,
            dma,
            dma((pieces,)),
            dma((pieces, sides)),
            dma((pieces, sides)),
            dma((pieces,)),
            dma((pieces,)),
            dma((STEPS,)),
            dma((STEPS, parts)),
            dma((STEPS,)),
            dma((STEPS,)),
            dma((STEPS,)),
            dma((STEPS,)),
        ],
        compiler_params=pltpu.CompilerParams(
            collective_id=0, has_side_effects=True, vmem_limit_bytes=63 * 1024 * 1024
        ),
    )(
        latents,
        neighbours.T,
        degree,
        send_rows.T,
        area,
        scenario,
        totals.T,
        w_send,
        w_recv,
        b_edge,
        w_msg,
        w_node,
        w_out,
        gain,
        w_dec,
        w_enc,
    )
    update = lax.dot_general(
        change, w_enc, (((0,), (0,)), ((), ())), preferred_element_type=F32
    )
    final = (latest.astype(F32) + update).astype(BF16)
    return final, jnp.transpose(conserved, (1, 0, 2))


def solution(mesh):
    every = ("members", "patch", "feat")
    group = ("patch", "feat")
    column = P(None, None, "feat")
    return jax.shard_map(
        functools.partial(shards, mesh.shape["patch"], mesh.shape["feat"]),
        mesh=mesh,
        in_specs=(
            P(every, None),
            P(group, None),
            P(group),
            P(group, None),
            P(group),
            P("members"),
            P(),
            column,
            column,
            P(),
            column,
            column,
            column,
            P(),
            P(),
            P(),
        ),
        out_specs=(P(every, None), P("members", None, group)),
        check_vma=False,
    )
```

```python
import functools

import jax
import jax.numpy as jnp
from jax import lax
from jax.experimental import pallas as pl
from jax.experimental.pallas import tpu as pltpu
from jax.sharding import PartitionSpec as P

STEPS = 2
EPSILON = 1e-05
DEAD = -1e30
MESH = pl.DeviceIdType.MESH
F32 = jnp.float32
BF16 = jnp.bfloat16
NT = (((1,), (1,)), ((), ()))


def mm(a, b):
    return jnp.dot(a, b, preferred_element_type=F32)


def half_silu(half):
    return half * jnp.tanh(half) + half


def softplus(x):
    return jnp.maximum(x, 0.0) + jnp.log1p(jnp.exp(-jnp.abs(x)))


def kernel(
    n_patch,
    n_feat,
    h_ref,
    nbr_ref,
    deg_ref,
    rows_ref,
    area_ref,
    scen_ref,
    tot_ref,
    ws_ref,
    wr_ref,
    be_ref,
    wm_ref,
    wn_ref,
    wo_ref,
    gain_ref,
    wd_ref,
    we_ref,
    out_ref,
    change_ref,
    cons_ref,
    w,
    ids,
    ohs,
    ohl,
    ohr,
    pre,
    table,
    recv_half,
    h_node,
    h_next,
    summed,
    send,
    recv,
    ar_src,
    ar_all,
    ax_src,
    ax_all,
    h_sem,
    out_sem,
    wl_sem,
    ws_sem,
    wr_sem,
    fs_sem,
    fr_sem,
    as_sem,
    ar_sem,
    ps_sem,
    pr_sem,
    xs_sem,
    xr_sem,
):
    nodes, width = h_ref.shape
    deg = nbr_ref.shape[0]
    slot = rows_ref.shape[0]
    groups, packed = pre.shape[0], pre.shape[1]
    few = packed // deg
    blocks, block = h_node.shape[0], h_node.shape[1]
    cols = ws_ref.shape[2]
    parts = ar_sem.shape[1]
    part_slots = n_patch // parts
    remote = n_patch * slot
    pieces = w.shape[0]
    unroll = 4 if groups % 4 == 0 else 1
    me = lax.axis_index("patch")
    feat = lax.axis_index("feat")
    core = lax.rem(me, 2)
    partner = me + 1 - 2 * core

    def peer(offset):
        return lax.rem(me + offset, n_patch)

    def side(offset):
        return lax.rem(feat + offset, n_feat)

    half = n_patch // 2
    depth = lax.div(me, 2)
    barrier = pltpu.get_barrier_semaphore()

    def greet(offset, carry):
        pl.semaphore_signal(barrier, inc=1, device_id={"patch": peer(offset)}, device_id_type=MESH)
        return carry

    def greet_pair(j, carry):
        return greet(half + j, greet(half - j, carry))

    greet(half, 0)
    lax.fori_loop(1, half, greet_pair, 0)
    for offset in range(1, n_feat):
        pl.semaphore_signal(barrier, inc=1, device_id={"feat": side(offset)}, device_id_type=MESH)

    span = width // 2
    mine = pl.ds(pl.multiple_of(core * span, span), span)
    low = mine
    high = pl.ds(pl.multiple_of(width + core * span, span), span)
    shards = (
        ws_ref.at[0, low],
        wr_ref.at[0, low],
        wn_ref.at[0, low],
        wm_ref.at[0, low],
        wn_ref.at[0, high],
        wo_ref.at[0, low],
    )

    def cols_of(owner):
        return pl.ds(pl.multiple_of(owner * cols, cols), cols)

    own_cols = cols_of(feat)
    load_h = pltpu.make_async_copy(h_ref, h_next, h_sem)
    local = [
        pltpu.make_async_copy(shards[i], w.at[i, mine, own_cols], wl_sem.at[i])
        for i in range(pieces)
    ]
    local[0].start()
    local[1].start()
    load_h.start()
    for i in range(2, pieces):
        local[i].start()

    def side_part(i, rows, owner, to, at):
        ref = w.at[i, rows, cols_of(owner)]
        return pltpu.make_async_remote_copy(
            src_ref=ref,
            dst_ref=ref,
            send_sem=ws_sem.at[i, at],
            recv_sem=wr_sem.at[i, at],
            device_id={"feat": to},
            device_id_type=MESH,
        )

    right, left = side(1), side(n_feat - 1)
    relay = n_feat == 4
    quart = span // 2
    rows_a = pl.ds(pl.multiple_of(core * span, quart), quart)
    rows_b = pl.ds(pl.multiple_of(core * span + quart, quart), quart)

    def first_copies(i):
        if relay:
            return [side_part(i, mine, feat, right, 0), side_part(i, mine, feat, left, 1)]
        return [side_part(i, mine, feat, side(o), o - 1) for o in range(1, n_feat)]

    def relay_copies(i):
        if relay:
            return [side_part(i, rows_a, left, right, 2), side_part(i, rows_b, right, left, 3)]
        return []

    def swap_copy(i):
        return pltpu.make_async_remote_copy(
            src_ref=w.at[i, mine],
            dst_ref=w.at[i, mine],
            send_sem=fs_sem.at[i],
            recv_sem=fr_sem.at[i],
            device_id={"patch": partner},
            device_id_type=MESH,
        )

    def own_out(i):
        local[i].wait()
        for copy in first_copies(i):
            copy.start()

    def pass_on(i):
        for copy in first_copies(i):
            copy.wait_recv()
        for copy in relay_copies(i):
            copy.start()

    def pass_over(i):
        for copy in relay_copies(i):
            copy.wait_recv()
        swap_copy(i).start()

    picks = rows_ref[...].T.astype(F32)
    spread = jnp.where(
        lax.broadcasted_iota(jnp.int32, (remote, n_patch), 0) // slot
        == lax.broadcasted_iota(jnp.int32, (remote, n_patch), 1),
        1.0,
        0.0,
    ).astype(BF16)
    coarse = jnp.floor(picks * (1.0 / 16.0))
    fine = picks - 16.0 * coarse
    each = mm(spread, coarse.astype(BF16)) * 16.0 + mm(spread, fine.astype(BF16))
    lane = lax.broadcasted_iota(jnp.int32, (remote, slot), 1)
    turn = lax.broadcasted_iota(jnp.int32, (remote, slot), 0) % slot
    chosen_row = jnp.sum(jnp.where(lane == turn, each, 0.0), axis=1, keepdims=True)
    node_at = lax.broadcasted_iota(jnp.int32, (remote, nodes), 1).astype(F32)
    ohs[...] = jnp.where(chosen_row == node_at, 1.0, 0.0).astype(BF16)

    def fill_send(step):
        picked = mm(ohs[...], h_next[...]).astype(BF16).reshape(n_patch, slot, width)
        send[step] = picked
        recv[step, pl.ds(n_patch - 1, 1)] = send[step, pl.ds(me, 1)]

    load_h.wait()
    fill_send(0)

    def slot_of(d):
        return jnp.where(d < 0, -2 * d - 1, 2 * d)

    def exchange(step, offset):
        target = peer(offset)
        place = slot_of(half - offset)
        pltpu.make_async_remote_copy(
            src_ref=send.at[step, target],
            dst_ref=recv.at[step, place],
            send_sem=as_sem.at[step],
            recv_sem=ar_sem.at[step, place // part_slots],
            device_id={"patch": target},
            device_id_type=MESH,
        ).start()

    def exchange_all(step):
        def body(j, carry):
            exchange(step, half - j)
            exchange(step, half + j)
            return carry

        exchange(step, half)
        lax.fori_loop(1, half, body, 0)

    def wait_part(step, g):
        count = part_slots - 1 if g == parts - 1 else part_slots
        ref = recv.at[step, pl.ds(0, count)]
        pltpu.make_async_copy(ref, ref, ar_sem.at[step, g]).wait()

    pl.semaphore_wait(barrier, n_patch - 1 + n_feat - 1)
    exchange_all(0)
    for i in range(pieces):
        own_out(i)
    pass_on(0)
    pass_on(1)

    raw = nbr_ref[...]
    far_id = jnp.maximum(raw - nodes, 0)
    source = far_id // slot - me
    source = jnp.where(source < 0, source + n_patch, source)
    ordered = jnp.where(raw < nodes, raw, nodes + slot_of(source - half) * slot + far_id % slot)
    live = lax.broadcasted_iota(jnp.int32, raw.shape, 0) < deg_ref[...].reshape(1, nodes)
    ids[...] = jnp.where(live, ordered, -1).T

    def select(g, carry):
        mine_ids = ids[pl.ds(g * few, few)]
        for k in range(deg):
            col = mine_ids[:, k : k + 1]
            for ref, base in ((ohl, 0), (ohr, nodes)):
                here = lax.broadcasted_iota(jnp.int32, (few, ref.shape[2]), 1) + base
                ref[g, pl.ds(k * few, few)] = jnp.where(col == here, 1.0, 0.0).astype(BF16)
        return carry

    lax.fori_loop(0, groups, select, 0)

    fields = wd_ref.shape[0]
    nodes_all = float(nodes * n_patch * n_feat)
    field_at = lax.broadcasted_iota(jnp.int32, tot_ref.shape, 0)
    wanted = jnp.zeros(tot_ref.shape, jnp.int32)
    for f in range(fields):
        wanted = jnp.where(field_at == f, scen_ref[f], wanted)
    scenario_at = lax.broadcasted_iota(jnp.int32, tot_ref.shape, 1)
    target = jnp.sum(jnp.where(scenario_at == wanted, tot_ref[...], 0.0), axis=1, keepdims=True)
    lanes = ar_src.shape[2]
    mark = lax.broadcasted_iota(jnp.int32, (fields, lanes), 0) == lax.broadcasted_iota(
        jnp.int32, (fields, lanes), 1
    )
    plane = 2 * n_feat
    seat = core * n_feat + feat

    def seat_copy(step, offset):
        other = lax.rem(seat + offset, plane)
        other_core = lax.div(other, n_feat)
        return pltpu.make_async_remote_copy(
            src_ref=ax_src.at[step],
            dst_ref=ax_all.at[step, seat],
            send_sem=xs_sem.at[step],
            recv_sem=xr_sem.at[step],
            device_id={"patch": me - core + other_core, "feat": lax.rem(other, n_feat)},
            device_id_type=MESH,
        )

    def wait_bytes(ref, sem):
        pltpu.make_async_copy(ref, ref, sem).wait()

    def put_sum(step, local_fields):
        area = area_ref[...].reshape(1, nodes)
        part = jnp.sum(local_fields * area, axis=1, keepdims=True)
        wide = jnp.broadcast_to(part, (fields, lanes))
        line = jnp.sum(jnp.where(mark, wide, 0.0), axis=0, keepdims=True)
        ar_src[step] = line
        ar_all[step, pl.ds(depth, 1)] = line.reshape(1, 1, lanes)

    def send_sum(step):
        def one(offset):
            pltpu.make_async_remote_copy(
                src_ref=ar_src.at[step],
                dst_ref=ar_all.at[step, depth],
                send_sem=ps_sem.at[step],
                recv_sem=pr_sem.at[step],
                device_id={"patch": peer(2 * offset)},
                device_id_type=MESH,
            ).start()

        middle = half // 2

        def both(j, carry):
            one(middle - j)
            one(middle + j)
            return carry

        one(middle)
        lax.fori_loop(1, middle, both, 0)

    def finish_sum(step):
        wait_bytes(ar_all.at[step, pl.ds(0, half - 1)], pr_sem.at[step])
        line = jnp.sum(ar_all[step], axis=0)
        ax_src[step] = line
        ax_all[step, pl.ds(seat, 1)] = line.reshape(1, 1, lanes)
        for offset in range(1, plane):
            seat_copy(step, offset).start()
        wait_bytes(ax_all.at[step, pl.ds(0, plane - 1)], xr_sem.at[step])
        line = jnp.sum(ax_all[step], axis=0)
        wide = jnp.broadcast_to(line, (fields, lanes))
        integral = jnp.sum(jnp.where(mark, wide, 0.0), axis=1, keepdims=True)
        return target * nodes_all / integral

    wd = wd_ref[...]

    def rescaled(rows, mix):
        part = softplus(lax.dot_general(rows, wd, NT, preferred_element_type=F32))
        change = jnp.dot(part, mix, precision=lax.Precision.HIGHEST, preferred_element_type=F32)
        return (rows.astype(F32) + change).astype(BF16)

    def project(b, carry):
        rows = pl.ds(b * block, block)
        latent = h_next[rows]
        table[rows] = (0.5 * mm(latent, w[0])).astype(BF16)
        recv_half[rows] = 0.5 * (mm(latent, w[1]) + be_ref[...])
        return carry

    def local_edges(t, carry):
        for u in range(unroll):
            g = t * unroll + u
            here = pl.ds(g * few, few)
            mine_ids = ids[here]
            base = recv_half[here]
            found = mm(ohl[g], table[pl.ds(0, nodes)])
            for k in range(deg):
                dead = jnp.where(mine_ids[:, k : k + 1] < 0, DEAD, 0.0)
                pre[g, pl.ds(k * few, few)] = found[k * few : (k + 1) * few] + (base + dead)
        return carry

    def node_part(b, carry):
        h_node[b] = mm(h_next[pl.ds(b * block, block)], w[2])
        return carry

    def remote_edges(t, carry):
        for u in range(unroll):
            g = t * unroll + u
            found = mm(ohr[g], table[pl.ds(nodes, remote)])
            total = jnp.zeros((few, width), F32)
            for k in range(deg):
                rows = pl.ds(k * few, few)
                total = total + half_silu(pre[g, rows] + found[k * few : (k + 1) * few])
            summed[pl.ds(g * few, few)] = total.astype(BF16)
        return carry

    def finish_block(b):
        rows = pl.ds(b * block, block)
        message = mm(summed[rows], w[3]).astype(BF16)
        hidden = half_silu(0.5 * (h_node[b] + mm(message, w[4]))).astype(BF16)
        output = mm(hidden, w[5])
        average = jnp.mean(output, axis=1, keepdims=True)
        centred = output - average
        variance = jnp.mean(jnp.square(centred), axis=1, keepdims=True)
        normed = centred * lax.rsqrt(variance + EPSILON) * gain_ref[...]
        h_next[rows] = (h_next[rows].astype(F32) + normed).astype(BF16)

    def place_part(step, g, mix):
        rows = recv[step, pl.ds(g * part_slots, part_slots)]
        rows = rows.reshape(part_slots * slot, width)
        if step > 0:
            rows = rescaled(rows, mix)
        at = pl.ds(nodes + g * part_slots * slot, part_slots * slot)
        table[at] = (0.5 * mm(rows, w[0])).astype(BF16)

    pass_over(0)
    pass_over(1)
    swap_copy(0).wait_recv()
    swap_copy(1).wait_recv()
    lax.fori_loop(0, blocks, project, 0)
    for i in range(2, pieces):
        pass_on(i)
    lax.fori_loop(0, groups // unroll, local_edges, 0)
    for i in range(2, pieces):
        pass_over(i)

    mix = None
    for step in range(STEPS):
        if step > 0:
            scale = finish_sum(step - 1)
            for f in range(fields):
                cons_ref[f, step - 1 : step] = (scale * local_fields)[f : f + 1]
            mix = (scale - 1.0) * we_ref[...]

            def move(b, carry):
                rows = pl.ds(b * block, block)
                h_next[rows] = rescaled(h_next[rows], mix)
                return carry

            lax.fori_loop(0, blocks, move, 0)
            lax.fori_loop(0, blocks, project, 0)
            lax.fori_loop(0, groups // unroll, local_edges, 0)
            lax.fori_loop(0, blocks, node_part, 0)

        for g in range(parts):
            wait_part(step, g)
            place_part(step, g, mix)
        lax.fori_loop(0, groups // unroll, remote_edges, 0)
        if step == 0:
            for i in range(2, pieces):
                swap_copy(i).wait_recv()
            lax.fori_loop(0, blocks, node_part, 0)
        for b in range(blocks):
            finish_block(b)

        if step + 1 == STEPS:
            give = pltpu.make_async_copy(h_next, out_ref, out_sem)
            give.start()
        local_fields = softplus(lax.dot_general(wd, h_next[...], NT, preferred_element_type=F32))
        put_sum(step, local_fields)
        if step + 1 < STEPS:
            fill_send(step + 1)
        send_sum(step)
        if step + 1 < STEPS:
            exchange_all(step + 1)

    scale = finish_sum(STEPS - 1)
    change_ref[...] = (scale - 1.0) * local_fields
    for f in range(fields):
        cons_ref[f, STEPS - 1 : STEPS] = (scale * local_fields)[f : f + 1]
    give.wait()

    for i in range(pieces):
        for copy in first_copies(i) + relay_copies(i):
            copy.wait_send()
        swap_copy(i).wait_send()
    for step in range(STEPS):
        wait_bytes(send.at[step, pl.ds(0, n_patch - 1)], as_sem.at[step])
        wait_bytes(ar_all.at[step, pl.ds(0, half - 1)], ps_sem.at[step])
        wait_bytes(ax_all.at[step, pl.ds(0, plane - 1)], xs_sem.at[step])


def shards(
    n_patch,
    n_feat,
    latents,
    neighbours,
    degree,
    send_rows,
    area,
    scenario,
    totals,
    w_send,
    w_recv,
    b_edge,
    w_msg,
    w_node,
    w_out,
    gain,
    w_dec,
    w_enc,
):
    nodes, width = latents.shape
    deg, slot = neighbours.shape[1], send_rows.shape[1]
    fields = w_dec.shape[0]
    block = min(256, nodes)
    blocks = nodes // block
    few = 32
    groups = nodes // few
    remote = n_patch * slot
    pieces = 6
    parts = 4
    lanes = 128
    sides = max(n_feat, 2)
    vmem = pl.BlockSpec(memory_space=pltpu.VMEM)
    smem = pl.BlockSpec(memory_space=pltpu.SMEM)
    hbm = pl.BlockSpec(memory_space=pltpu.HBM)
    dma = pltpu.SemaphoreType.DMA
    latest, change, conserved = pl.pallas_call(
        functools.partial(kernel, n_patch, n_feat),
        out_shape=(
            jax.ShapeDtypeStruct((nodes, width), BF16),
            jax.ShapeDtypeStruct((fields, nodes), F32),
            jax.ShapeDtypeStruct((fields, STEPS, nodes), F32),
        ),
        in_specs=[hbm, vmem, vmem, vmem, vmem, smem, vmem, hbm, hbm, vmem, hbm, hbm, hbm]
        + [vmem] * 3,
        out_specs=(hbm, vmem, vmem),
        scratch_shapes=[
            pltpu.VMEM((pieces, width, width), BF16),
            pltpu.VMEM((nodes, deg), jnp.int32),
            pltpu.VMEM((remote, nodes), BF16),
            pltpu.VMEM((groups, deg * few, nodes), BF16),
            pltpu.VMEM((groups, deg * few, remote), BF16),
            pltpu.VMEM((groups, deg * few, width), F32),
            pltpu.VMEM((nodes + remote, width), BF16),
            pltpu.VMEM((nodes, width), F32),
            pltpu.VMEM((blocks, block, width), F32),
            pltpu.VMEM((nodes, width), BF16),
            pltpu.VMEM((nodes, width), BF16),
            pltpu.VMEM((STEPS, n_patch, slot, width), BF16),
            pltpu.VMEM((STEPS, n_patch, slot, width), BF16),
            pltpu.VMEM((STEPS, 1, lanes), F32),
            pltpu.VMEM((STEPS, n_patch // 2, 1, lanes), F32),
            pltpu.VMEM((STEPS, 1, lanes), F32),
            pltpu.VMEM((STEPS, 2 * n_feat, 1, lanes), F32),
            dma,
            dma,
            dma((pieces,)),
            dma((pieces, sides)),
            dma((pieces, sides)),
            dma((pieces,)),
            dma((pieces,)),
            dma((STEPS,)),
            dma((STEPS, parts)),
            dma((STEPS,)),
            dma((STEPS,)),
            dma((STEPS,)),
            dma((STEPS,)),
        ],
        compiler_params=pltpu.CompilerParams(
            collective_id=0, has_side_effects=True, vmem_limit_bytes=63 * 1024 * 1024
        ),
    )(
        latents,
        neighbours.T,
        degree,
        send_rows.T,
        area,
        scenario,
        totals.T,
        w_send,
        w_recv,
        b_edge,
        w_msg,
        w_node,
        w_out,
        gain,
        w_dec,
        w_enc,
    )
    update = lax.dot_general(
        change, w_enc, (((0,), (0,)), ((), ())), preferred_element_type=F32
    )
    final = (latest.astype(F32) + update).astype(BF16)
    return final, jnp.transpose(conserved, (1, 0, 2))


def solution(mesh):
    every = ("members", "patch", "feat")
    group = ("patch", "feat")
    column = P(None, None, "feat")
    return jax.shard_map(
        functools.partial(shards, mesh.shape["patch"], mesh.shape["feat"]),
        mesh=mesh,
        in_specs=(
            P(every, None),
            P(group, None),
            P(group),
            P(group, None),
            P(group),
            P("members"),
            P(),
            column,
            column,
            P(),
            column,
            column,
            column,
            P(),
            P(),
            P(),
        ),
        out_specs=(P(every, None), P("members", None, group)),
        check_vma=False,
    )
```

```python
import functools

import jax
import jax.numpy as jnp
from jax import lax
from jax.experimental import pallas as pl
from jax.experimental.pallas import tpu as pltpu
from jax.sharding import PartitionSpec as P

STEPS = 2
EPSILON = 1e-05
DEAD = -1e30
MESH = pl.DeviceIdType.MESH
F32 = jnp.float32
BF16 = jnp.bfloat16
NT = (((1,), (1,)), ((), ()))


def mm(a, b):
    return jnp.dot(a, b, preferred_element_type=F32)


def half_silu(half):
    return half * jnp.tanh(half) + half


def softplus(x):
    return jnp.maximum(x, 0.0) + jnp.log1p(jnp.exp(-jnp.abs(x)))


def kernel(
    n_patch,
    n_feat,
    h_ref,
    nbr_ref,
    deg_ref,
    rows_ref,
    area_ref,
    scen_ref,
    tot_ref,
    ws_ref,
    wr_ref,
    be_ref,
    wm_ref,
    wn_ref,
    wo_ref,
    gain_ref,
    wd_ref,
    we_ref,
    out_ref,
    change_ref,
    cons_ref,
    w,
    ids,
    ohs,
    ohl,
    ohr,
    pre,
    table,
    recv_half,
    h_node,
    h_next,
    summed,
    send,
    recv,
    ar_src,
    ar_all,
    ax_src,
    ax_all,
    in_sem,
    token_sem,
    pair_sem,
    h_sem,
    out_sem,
    wl_sem,
    ws_sem,
    wr_sem,
    fs_sem,
    fr_sem,
    as_sem,
    ar_sem,
    ps_sem,
    pr_sem,
    xs_sem,
    xr_sem,
):
    nodes, width = h_ref.shape
    deg = nbr_ref.shape[0]
    slot = rows_ref.shape[0]
    groups, packed = pre.shape[0], pre.shape[1]
    few = packed // deg
    blocks, block = h_node.shape[0], h_node.shape[1]
    cols = ws_ref.shape[2]
    parts = ar_sem.shape[1]
    part_slots = n_patch // parts
    remote = n_patch * slot
    pieces = w.shape[0]
    unroll = 4 if groups % 4 == 0 else 1
    me = lax.axis_index("patch")
    feat = lax.axis_index("feat")
    core = lax.rem(me, 2)
    partner = me + 1 - 2 * core

    def peer(offset):
        return lax.rem(me + offset, n_patch)

    def side(offset):
        return lax.rem(feat + offset, n_feat)

    rank = lax.rem(me + n_patch - 1, n_patch)
    half = n_patch // 2
    depth = lax.div(me, 2)
    ahead = peer(2)
    behind = peer(n_patch - 2)
    first = jnp.where(core == 1, 0, 1)
    last = jnp.where(core == 1, half - 1, 0)
    paired = depth > 0
    barrier = pltpu.get_barrier_semaphore()

    def greet(**device):
        pl.semaphore_signal(barrier, inc=1, device_id=device, device_id_type=MESH)

    @pl.when(depth != first)
    def _():
        greet(patch=behind)

    @pl.when(paired)
    def _():
        greet(patch=partner)

    for offset in range(1, n_feat):
        greet(feat=side(offset))

    span = width // 2
    mine = pl.ds(pl.multiple_of(core * span, span), span)
    low = mine
    high = pl.ds(pl.multiple_of(width + core * span, span), span)
    shards = (
        ws_ref.at[0, low],
        wr_ref.at[0, low],
        wn_ref.at[0, low],
        wm_ref.at[0, low],
        wn_ref.at[0, high],
        wo_ref.at[0, low],
    )

    def cols_of(owner):
        return pl.ds(pl.multiple_of(owner * cols, cols), cols)

    own_cols = cols_of(feat)
    load_h = pltpu.make_async_copy(h_ref, h_next, h_sem)
    local = [
        pltpu.make_async_copy(shards[i], w.at[i, mine, own_cols], wl_sem.at[i])
        for i in range(pieces)
    ]
    local[0].start()
    local[1].start()
    load_h.start()
    for i in range(2, pieces):
        local[i].start()

    greetings = n_feat - 1 + jnp.where(depth != last, 1, 0) + jnp.where(paired, 1, 0)
    pl.semaphore_wait(barrier, greetings)
    closing = me == n_patch - 2

    def tell_ahead():
        pl.semaphore_signal(token_sem, inc=1, device_id={"patch": ahead}, device_id_type=MESH)

    @pl.when(depth != first)
    def _():
        pl.semaphore_wait(token_sem, 1)

    @pl.when(jnp.logical_and(depth != last, jnp.logical_not(closing)))
    def _():
        tell_ahead()

    @pl.when(paired)
    def _():
        pl.semaphore_signal(pair_sem, inc=1, device_id={"patch": partner}, device_id_type=MESH)
        pl.semaphore_wait(pair_sem, 1)

    @pl.when(closing)
    def _():
        tell_ahead()

    def arrive(offset):
        @pl.when(rank + offset >= n_patch)
        def _():
            pl.semaphore_signal(
                in_sem.at[rank],
                inc=1,
                device_id={"patch": peer(offset)},
                device_id_type=MESH,
            )

    def arrive_pair(j, carry):
        arrive(half - j)
        arrive(half + j)
        return carry

    arrive(half)
    lax.fori_loop(1, half, arrive_pair, 0)

    def side_part(i, rows, owner, to, at):
        ref = w.at[i, rows, cols_of(owner)]
        return pltpu.make_async_remote_copy(
            src_ref=ref,
            dst_ref=ref,
            send_sem=ws_sem.at[i, at],
            recv_sem=wr_sem.at[i, at],
            device_id={"feat": to},
            device_id_type=MESH,
        )

    right, left = side(1), side(n_feat - 1)
    relay = n_feat == 4
    quart = span // 2
    rows_a = pl.ds(pl.multiple_of(core * span, quart), quart)
    rows_b = pl.ds(pl.multiple_of(core * span + quart, quart), quart)

    def first_copies(i):
        if relay:
            return [side_part(i, mine, feat, right, 0), side_part(i, mine, feat, left, 1)]
        return [side_part(i, mine, feat, side(o), o - 1) for o in range(1, n_feat)]

    def relay_copies(i):
        if relay:
            return [side_part(i, rows_a, left, right, 2), side_part(i, rows_b, right, left, 3)]
        return []

    def swap_copy(i):
        return pltpu.make_async_remote_copy(
            src_ref=w.at[i, mine],
            dst_ref=w.at[i, mine],
            send_sem=fs_sem.at[i],
            recv_sem=fr_sem.at[i],
            device_id={"patch": partner},
            device_id_type=MESH,
        )

    def own_out(i):
        local[i].wait()
        for copy in first_copies(i):
            copy.start()

    def pass_on(i):
        for copy in first_copies(i):
            copy.wait_recv()
        for copy in relay_copies(i):
            copy.start()

    def pass_over(i):
        for copy in relay_copies(i):
            copy.wait_recv()
        swap_copy(i).start()

    picks = rows_ref[...].T.astype(F32)
    spread = jnp.where(
        lax.broadcasted_iota(jnp.int32, (remote, n_patch), 0) // slot
        == lax.broadcasted_iota(jnp.int32, (remote, n_patch), 1),
        1.0,
        0.0,
    ).astype(BF16)
    coarse = jnp.floor(picks * (1.0 / 16.0))
    fine = picks - 16.0 * coarse
    each = mm(spread, coarse.astype(BF16)) * 16.0 + mm(spread, fine.astype(BF16))
    lane = lax.broadcasted_iota(jnp.int32, (remote, slot), 1)
    turn = lax.broadcasted_iota(jnp.int32, (remote, slot), 0) % slot
    chosen_row = jnp.sum(jnp.where(lane == turn, each, 0.0), axis=1, keepdims=True)
    node_at = lax.broadcasted_iota(jnp.int32, (remote, nodes), 1).astype(F32)
    ohs[...] = jnp.where(chosen_row == node_at, 1.0, 0.0).astype(BF16)

    def fill_send(step):
        picked = mm(ohs[...], h_next[...]).astype(BF16).reshape(n_patch, slot, width)
        send[step] = picked
        recv[step, pl.ds(n_patch - 1, 1)] = send[step, pl.ds(me, 1)]

    load_h.wait()
    fill_send(0)
    own_out(0)
    own_out(1)

    def slot_of(d):
        return jnp.where(d < 0, -2 * d - 1, 2 * d)

    def exchange(step, offset):
        target = peer(offset)
        place = slot_of(half - offset)
        pltpu.make_async_remote_copy(
            src_ref=send.at[step, target],
            dst_ref=recv.at[step, place],
            send_sem=as_sem.at[step],
            recv_sem=ar_sem.at[step, place // part_slots],
            device_id={"patch": target},
            device_id_type=MESH,
        ).start()

    def exchange_first(step):
        exchange(step, half)
        exchange(step, half - 1)
        exchange(step, half + 1)

    def exchange_rest(step):
        def body(j, carry):
            exchange(step, half - j)
            exchange(step, half + j)
            return carry

        lax.fori_loop(2, half, body, 0)

    def wait_part(step, g):
        count = part_slots - 1 if g == parts - 1 else part_slots
        ref = recv.at[step, pl.ds(0, count)]
        pltpu.make_async_copy(ref, ref, ar_sem.at[step, g]).wait()

    def send_back(offset):
        @pl.when(rank + offset >= n_patch)
        def _():
            exchange(0, offset)

    def send_back_pair(j, carry):
        send_back(half - j)
        send_back(half + j)
        return carry

    def send_ahead(on, carry):
        pl.semaphore_wait(in_sem.at[rank + on], 1)
        exchange(0, on)
        return carry

    send_back(half)
    lax.fori_loop(1, half, send_back_pair, 0)
    pass_on(0)
    pass_on(1)
    for i in range(2, pieces):
        own_out(i)
    lax.fori_loop(1, n_patch - rank, send_ahead, 0)

    raw = nbr_ref[...]
    far_id = jnp.maximum(raw - nodes, 0)
    source = far_id // slot - me
    source = jnp.where(source < 0, source + n_patch, source)
    ordered = jnp.where(raw < nodes, raw, nodes + slot_of(source - half) * slot + far_id % slot)
    live = lax.broadcasted_iota(jnp.int32, raw.shape, 0) < deg_ref[...].reshape(1, nodes)
    ids[...] = jnp.where(live, ordered, -1).T

    def select(g, carry):
        mine_ids = ids[pl.ds(g * few, few)]
        for k in range(deg):
            col = mine_ids[:, k : k + 1]
            for ref, base in ((ohl, 0), (ohr, nodes)):
                here = lax.broadcasted_iota(jnp.int32, (few, ref.shape[2]), 1) + base
                ref[g, pl.ds(k * few, few)] = jnp.where(col == here, 1.0, 0.0).astype(BF16)
        return carry

    lax.fori_loop(0, groups, select, 0)

    fields = wd_ref.shape[0]
    nodes_all = float(nodes * n_patch * n_feat)
    field_at = lax.broadcasted_iota(jnp.int32, tot_ref.shape, 0)
    wanted = jnp.zeros(tot_ref.shape, jnp.int32)
    for f in range(fields):
        wanted = jnp.where(field_at == f, scen_ref[f], wanted)
    scenario_at = lax.broadcasted_iota(jnp.int32, tot_ref.shape, 1)
    target = jnp.sum(jnp.where(scenario_at == wanted, tot_ref[...], 0.0), axis=1, keepdims=True)
    lanes = ar_src.shape[2]
    mark = lax.broadcasted_iota(jnp.int32, (fields, lanes), 0) == lax.broadcasted_iota(
        jnp.int32, (fields, lanes), 1
    )
    plane = 2 * n_feat
    seat = core * n_feat + feat

    def seat_copy(step, offset):
        other = lax.rem(seat + offset, plane)
        other_core = lax.div(other, n_feat)
        return pltpu.make_async_remote_copy(
            src_ref=ax_src.at[step],
            dst_ref=ax_all.at[step, seat],
            send_sem=xs_sem.at[step],
            recv_sem=xr_sem.at[step],
            device_id={"patch": me - core + other_core, "feat": lax.rem(other, n_feat)},
            device_id_type=MESH,
        )

    def wait_bytes(ref, sem):
        pltpu.make_async_copy(ref, ref, sem).wait()

    def put_sum(step, local_fields):
        area = area_ref[...].reshape(1, nodes)
        part = jnp.sum(local_fields * area, axis=1, keepdims=True)
        wide = jnp.broadcast_to(part, (fields, lanes))
        line = jnp.sum(jnp.where(mark, wide, 0.0), axis=0, keepdims=True)
        ar_src[step] = line
        ar_all[step, pl.ds(depth, 1)] = line.reshape(1, 1, lanes)

    def send_sum(step):
        def one(offset):
            pltpu.make_async_remote_copy(
                src_ref=ar_src.at[step],
                dst_ref=ar_all.at[step, depth],
                send_sem=ps_sem.at[step],
                recv_sem=pr_sem.at[step],
                device_id={"patch": peer(2 * offset)},
                device_id_type=MESH,
            ).start()

        middle = half // 2

        def both(j, carry):
            one(middle - j)
            one(middle + j)
            return carry

        one(middle)
        lax.fori_loop(1, middle, both, 0)

    def finish_sum(step):
        wait_bytes(ar_all.at[step, pl.ds(0, half - 1)], pr_sem.at[step])
        line = jnp.sum(ar_all[step], axis=0)
        ax_src[step] = line
        ax_all[step, pl.ds(seat, 1)] = line.reshape(1, 1, lanes)
        for offset in range(1, plane):
            seat_copy(step, offset).start()
        wait_bytes(ax_all.at[step, pl.ds(0, plane - 1)], xr_sem.at[step])
        line = jnp.sum(ax_all[step], axis=0)
        wide = jnp.broadcast_to(line, (fields, lanes))
        integral = jnp.sum(jnp.where(mark, wide, 0.0), axis=1, keepdims=True)
        return target * nodes_all / integral

    wd = wd_ref[...]

    def rescaled(rows, mix):
        part = softplus(lax.dot_general(rows, wd, NT, preferred_element_type=F32))
        change = jnp.dot(part, mix, precision=lax.Precision.HIGHEST, preferred_element_type=F32)
        return (rows.astype(F32) + change).astype(BF16)

    def project(b, carry):
        rows = pl.ds(b * block, block)
        latent = h_next[rows]
        table[rows] = (0.5 * mm(latent, w[0])).astype(BF16)
        recv_half[rows] = 0.5 * (mm(latent, w[1]) + be_ref[...])
        return carry

    def local_edges(t, carry):
        for u in range(unroll):
            g = t * unroll + u
            here = pl.ds(g * few, few)
            mine_ids = ids[here]
            base = recv_half[here]
            found = mm(ohl[g], table[pl.ds(0, nodes)])
            for k in range(deg):
                dead = jnp.where(mine_ids[:, k : k + 1] < 0, DEAD, 0.0)
                pre[g, pl.ds(k * few, few)] = found[k * few : (k + 1) * few] + (base + dead)
        return carry

    def node_part(b, carry):
        h_node[b] = mm(h_next[pl.ds(b * block, block)], w[2])
        return carry

    fan = remote // 2

    def far_edges(t, carry):
        for u in range(unroll):
            g = t * unroll + u
            pre[g] += mm(ohr[g, :, pl.ds(0, fan)], table[pl.ds(nodes, fan)])
        return carry

    def near_edges(t, carry):
        for u in range(unroll):
            g = t * unroll + u
            found = mm(ohr[g, :, pl.ds(fan, fan)], table[pl.ds(nodes + fan, fan)])
            total = jnp.zeros((few, width), F32)
            for k in range(deg):
                rows = pl.ds(k * few, few)
                total = total + half_silu(pre[g, rows] + found[k * few : (k + 1) * few])
            summed[pl.ds(g * few, few)] = total.astype(BF16)
        return carry

    def finish_block(b):
        rows = pl.ds(b * block, block)
        message = mm(summed[rows], w[3]).astype(BF16)
        hidden = half_silu(0.5 * (h_node[b] + mm(message, w[4]))).astype(BF16)
        output = mm(hidden, w[5])
        average = jnp.mean(output, axis=1, keepdims=True)
        centred = output - average
        variance = jnp.mean(jnp.square(centred), axis=1, keepdims=True)
        normed = centred * lax.rsqrt(variance + EPSILON) * gain_ref[...]
        h_next[rows] = (h_next[rows].astype(F32) + normed).astype(BF16)

    def place_part(step, g, mix):
        rows = recv[step, pl.ds(g * part_slots, part_slots)]
        rows = rows.reshape(part_slots * slot, width)
        if step > 0:
            rows = rescaled(rows, mix)
        at = pl.ds(nodes + g * part_slots * slot, part_slots * slot)
        table[at] = (0.5 * mm(rows, w[0])).astype(BF16)

    pass_over(0)
    pass_over(1)
    swap_copy(0).wait_recv()
    swap_copy(1).wait_recv()
    lax.fori_loop(0, blocks, project, 0)
    for i in range(2, pieces):
        pass_on(i)
    lax.fori_loop(0, groups // unroll, local_edges, 0)
    for i in range(2, pieces):
        pass_over(i)
    for i in range(2, pieces):
        swap_copy(i).wait_recv()
    lax.fori_loop(0, blocks, node_part, 0)

    mix = None
    for step in range(STEPS):
        if step > 0:
            scale = finish_sum(step - 1)
            for f in range(fields):
                cons_ref[f, step - 1 : step] = (scale * local_fields)[f : f + 1]
            mix = (scale - 1.0) * we_ref[...]

            def move(b, carry):
                rows = pl.ds(b * block, block)
                h_next[rows] = rescaled(h_next[rows], mix)
                return carry

            lax.fori_loop(0, blocks, move, 0)
            lax.fori_loop(0, blocks, project, 0)
            lax.fori_loop(0, groups // unroll, local_edges, 0)
            lax.fori_loop(0, blocks, node_part, 0)

        for g in range(parts):
            wait_part(step, g)
            place_part(step, g, mix)
            if g == parts // 2 - 1:
                lax.fori_loop(0, groups // unroll, far_edges, 0)
        lax.fori_loop(0, groups // unroll, near_edges, 0)
        for b in range(blocks):
            finish_block(b)

        if step + 1 == STEPS:
            give = pltpu.make_async_copy(h_next, out_ref, out_sem)
            give.start()
        else:
            fill_send(step + 1)
        local_fields = softplus(lax.dot_general(wd, h_next[...], NT, preferred_element_type=F32))
        if step + 1 < STEPS:
            exchange_first(step + 1)
        put_sum(step, local_fields)
        send_sum(step)
        if step + 1 < STEPS:
            exchange_rest(step + 1)

    scale = finish_sum(STEPS - 1)
    change_ref[...] = (scale - 1.0) * local_fields
    for f in range(fields):
        cons_ref[f, STEPS - 1 : STEPS] = (scale * local_fields)[f : f + 1]
    give.wait()

    for i in range(pieces):
        for copy in first_copies(i) + relay_copies(i):
            copy.wait_send()
        swap_copy(i).wait_send()
    for step in range(STEPS):
        wait_bytes(send.at[step, pl.ds(0, n_patch - 1)], as_sem.at[step])
        wait_bytes(ar_all.at[step, pl.ds(0, half - 1)], ps_sem.at[step])
        wait_bytes(ax_all.at[step, pl.ds(0, plane - 1)], xs_sem.at[step])


def shards(
    n_patch,
    n_feat,
    latents,
    neighbours,
    degree,
    send_rows,
    area,
    scenario,
    totals,
    w_send,
    w_recv,
    b_edge,
    w_msg,
    w_node,
    w_out,
    gain,
    w_dec,
    w_enc,
):
    nodes, width = latents.shape
    deg, slot = neighbours.shape[1], send_rows.shape[1]
    fields = w_dec.shape[0]
    block = min(256, nodes)
    blocks = nodes // block
    few = 32
    groups = nodes // few
    remote = n_patch * slot
    pieces = 6
    parts = 4
    lanes = 128
    sides = max(n_feat, 2)
    vmem = pl.BlockSpec(memory_space=pltpu.VMEM)
    smem = pl.BlockSpec(memory_space=pltpu.SMEM)
    hbm = pl.BlockSpec(memory_space=pltpu.HBM)
    dma = pltpu.SemaphoreType.DMA
    latest, change, conserved = pl.pallas_call(
        functools.partial(kernel, n_patch, n_feat),
        out_shape=(
            jax.ShapeDtypeStruct((nodes, width), BF16),
            jax.ShapeDtypeStruct((fields, nodes), F32),
            jax.ShapeDtypeStruct((fields, STEPS, nodes), F32),
        ),
        in_specs=[hbm, vmem, vmem, vmem, vmem, smem, vmem, hbm, hbm, vmem, hbm, hbm, hbm]
        + [vmem] * 3,
        out_specs=(hbm, vmem, vmem),
        scratch_shapes=[
            pltpu.VMEM((pieces, width, width), BF16),
            pltpu.VMEM((nodes, deg), jnp.int32),
            pltpu.VMEM((remote, nodes), BF16),
            pltpu.VMEM((groups, deg * few, nodes), BF16),
            pltpu.VMEM((groups, deg * few, remote), BF16),
            pltpu.VMEM((groups, deg * few, width), F32),
            pltpu.VMEM((nodes + remote, width), BF16),
            pltpu.VMEM((nodes, width), F32),
            pltpu.VMEM((blocks, block, width), F32),
            pltpu.VMEM((nodes, width), BF16),
            pltpu.VMEM((nodes, width), BF16),
            pltpu.VMEM((STEPS, n_patch, slot, width), BF16),
            pltpu.VMEM((STEPS, n_patch, slot, width), BF16),
            pltpu.VMEM((STEPS, 1, lanes), F32),
            pltpu.VMEM((STEPS, n_patch // 2, 1, lanes), F32),
            pltpu.VMEM((STEPS, 1, lanes), F32),
            pltpu.VMEM((STEPS, 2 * n_feat, 1, lanes), F32),
            pltpu.SemaphoreType.REGULAR((n_patch,)),
            pltpu.SemaphoreType.REGULAR,
            pltpu.SemaphoreType.REGULAR,
            dma,
            dma,
            dma((pieces,)),
            dma((pieces, sides)),
            dma((pieces, sides)),
            dma((pieces,)),
            dma((pieces,)),
            dma((STEPS,)),
            dma((STEPS, parts)),
            dma((STEPS,)),
            dma((STEPS,)),
            dma((STEPS,)),
            dma((STEPS,)),
        ],
        compiler_params=pltpu.CompilerParams(
            collective_id=0, has_side_effects=True, vmem_limit_bytes=63 * 1024 * 1024
        ),
    )(
        latents,
        neighbours.T,
        degree,
        send_rows.T,
        area,
        scenario,
        totals.T,
        w_send,
        w_recv,
        b_edge,
        w_msg,
        w_node,
        w_out,
        gain,
        w_dec,
        w_enc,
    )
    update = lax.dot_general(
        change, w_enc, (((0,), (0,)), ((), ())), preferred_element_type=F32
    )
    final = (latest.astype(F32) + update).astype(BF16)
    return final, jnp.transpose(conserved, (1, 0, 2))


def solution(mesh):
    every = ("members", "patch", "feat")
    group = ("patch", "feat")
    column = P(None, None, "feat")
    return jax.shard_map(
        functools.partial(shards, mesh.shape["patch"], mesh.shape["feat"]),
        mesh=mesh,
        in_specs=(
            P(every, None),
            P(group, None),
            P(group),
            P(group, None),
            P(group),
            P("members"),
            P(),
            column,
            column,
            P(),
            column,
            column,
            column,
            P(),
            P(),
            P(),
        ),
        out_specs=(P(every, None), P("members", None, group)),
        check_vma=False,
    )
```
